256 devices in a mesh: cuts: 16 (over z_lo, y, core), sub: 16 (over z_hi, x).
Axes of the slice: x: 4, y: 4, z: 8 (z_hi: 4, z_lo: 2; z = z_hi * 2 + z_lo), core: 2. Of those that a mesh axis runs over, the one named last changes fastest.
Arguments:
- start_states: float32 [16, 32, 512, 128], P('cuts', 'sub'), may hold values from -8 to 8
- source: bfloat16 [32, 512, 128], P('sub'), may hold values from -3 to 3
- block_inverse: bfloat16 [32, 512, 512], P('sub'), may hold values from -1 to 1
- face_map: int32 [32, 2, 128], P('sub'), may hold values from 0 to 127, each once within a row
- transmissibility: float32 [32, 2, 128], P('sub'), may hold values from 7 to 11
- partner: int32 [32], replicated, may hold values from 0 to 31
- fracture_cond: float32 [32], replicated, may hold values from 0.3 to 3
Outputs:
- new_starts: float32 [16, 32, 512, 128], P('cuts', 'sub')
The draws below stay inside these ranges and needn't reach their ends.
All inputs are finite; a program needn't handle non-finite values.
Results may differ from the reference program's by a relative error of at most 0.0024.
Values sent between devices are 32-bit elements; how exact they have to be, the bound alone decides.
A program may use at most 64 MiB of HBM per device.

```python
import math
import jax
import jax.numpy as jnp
from jax import lax

BLOCK = 512
FACE = 128
SCENARIOS = 128
FINE_STEPS = 4
SWEEPS = 4
SLICES = 16
BLOCKS = 32


def draw_block_inverse(key, part):
    first, second = jax.random.split(jax.random.fold_in(key, 11))
    noise = jnp.clip(jax.random.normal(first, (BLOCKS, BLOCK, BLOCK), jnp.float32), -4.0, 4.0)
    diag_gain = jax.random.uniform(second, (BLOCKS, BLOCK), jnp.float32, 0.9, 1.1)
    places = jnp.arange(BLOCK, dtype=jnp.int32)
    on_face = jnp.logical_or(places < FACE, places >= BLOCK - FACE)
    diag_value = jnp.where(on_face[None, :], 0.07, 0.6) * diag_gain
    root = jnp.sqrt(diag_value)
    eye = jnp.eye(BLOCK, dtype=jnp.float32)
    inner = eye[None] + 0.25 * noise / jnp.sqrt(1.0 * BLOCK)
    matrix = root[:, :, None] * inner * root[:, None, :]
    return matrix.astype(jnp.bfloat16)


def draw_start_states(key, part):
    first, second = jax.random.split(jax.random.fold_in(key, 23), 2)
    offset = jax.random.normal(first, (SLICES, BLOCKS, 1, SCENARIOS), jnp.float32)
    noise = 0.5 * jax.random.normal(second, (SLICES, BLOCKS, BLOCK, SCENARIOS), jnp.float32)
    return jnp.clip(offset + noise, -8.0, 8.0)


def touch_ends(entries, rng, least, high):
    longest = entries.shape.index(max(entries.shape))
    spots = []
    for shift in (0, 1):
        where = [jax.random.randint(jax.random.fold_in(rng, axis), (), 0, length) for axis, length in enumerate(entries.shape)]
        where[longest] = (where[longest] + shift) % entries.shape[longest]
        spots.append(tuple(where))
    return entries.at[spots[0]].set(least).at[spots[1]].set(high)


def levels(own_key, extent, cuts, smallest, high):
    gain, own = 1.0, jax.random.fold_in(own_key, 6)
    for position, parts in cuts:
        draws = jnp.exp(jax.random.uniform(jax.random.fold_in(own, position), (parts,), jnp.float32, smallest / len(cuts), high / len(cuts)))
        gain = gain * jnp.repeat(draws, extent[position] // parts).reshape([-1 if axis == position else 1 for axis in range(len(extent))])
    return gain


def normal_values(own_key, extent, scale, limit, shards=(), held_as=jnp.bfloat16):
    entries = scale * jax.random.normal(own_key, extent, jnp.float32)
    if shards:
        entries = entries * levels(own_key, extent, shards, -0.22, 0.18)
    return jnp.clip(entries, -limit, limit).astype(held_as)


def setup_inputs(seed: int = 0) -> dict:
    seeds = jax.random.split(jax.random.key(seed), 8)
    start_states = draw_start_states(jax.random.fold_in(seeds[7], 71), 0)
    source = normal_values(seeds[1], (BLOCKS, BLOCK, SCENARIOS), 0.5, 3.0, ((0, 16),))
    block_inverse = draw_block_inverse(jax.random.fold_in(seeds[7], 71), 0)
    face_map = jax.vmap(lambda own: jax.random.permutation(own, FACE))(jax.random.split(seeds[3], BLOCKS * 2)).reshape((BLOCKS, 2, FACE)).astype(jnp.int32)
    transmissibility = jnp.clip(jnp.exp(math.log(11.0) - 0.45198512 * jax.random.uniform(seeds[4], (BLOCKS, 2, FACE), jnp.float32) ** levels(seeds[4], (BLOCKS, 2, FACE), ((0, 16),), -0.2, 0.2)), 7.0, 11.0)
    partner = touch_ends(jax.random.randint(seeds[5], (BLOCKS,), 0, BLOCKS), jax.random.fold_in(seeds[5], 1), 0, BLOCKS - 1).astype(jnp.int32)
    fracture_cond = jnp.clip(jnp.exp(jax.random.uniform(seeds[6], (BLOCKS,), jnp.float32, math.log(0.3), math.log(3.0))), 0.3, 3.0)
    return dict(start_states=start_states, source=source, block_inverse=block_inverse, face_map=face_map, transmissibility=transmissibility, partner=partner, fracture_cond=fracture_cond)


def face_terms(below, above, face_map, transmissibility):
    low_in = transmissibility[:, 0, :, None] * jnp.take_along_axis(below, face_map[:, 0, :, None], axis=1)
    up_in = transmissibility[:, 1, :, None] * jnp.take_along_axis(above, face_map[:, 1, :, None], axis=1)
    return (low_in, up_in)

def sweep(state, rhs, inverse_wide, face_map, transmissibility):
    lower = state[:, :FACE]
    upper = state[:, BLOCK - FACE:]
    zero = jnp.zeros_like(upper[:1])
    below = jnp.concatenate([zero, upper[:-1]], axis=0)
    above = jnp.concatenate([lower[1:], zero], axis=0)
    low_in, up_in = face_terms(below, above, face_map, transmissibility)
    full = jnp.concatenate([rhs[:, :FACE] + low_in, rhs[:, FACE:BLOCK - FACE], rhs[:, BLOCK - FACE:] + up_in], axis=1)
    full = full.astype(jnp.bfloat16).astype(jnp.float32)
    return jnp.einsum('bij,bjr->bir', inverse_wide, full)

def coarse_map(partner, fracture_cond):
    count = partner.shape[0]
    places = jnp.arange(count, dtype=jnp.int32)
    chain = (jnp.abs(places[:, None] - places[None, :]) == 1).astype(jnp.float32)
    onehot = (partner[:, None] == places[None, :]).astype(jnp.float32)
    linked = fracture_cond[:, None] * onehot
    weights = chain + linked + linked.T
    lapl = jnp.diag(jnp.sum(weights, axis=1)) - weights
    system = jnp.eye(count, dtype=jnp.float32) + lapl
    factor = jnp.linalg.cholesky(system)
    return jax.scipy.linalg.cho_solve((factor, True), jnp.eye(count, dtype=jnp.float32))

def reference(start_states, source, block_inverse, face_map, transmissibility, partner, fracture_cond):
    inverse_wide = block_inverse.astype(jnp.float32)
    source_wide = source.astype(jnp.float32)

    def propagate(start):
        state = start
        for step in range(FINE_STEPS):
            rhs = state + source_wide
            for turn in range(SWEEPS):
                state = sweep(state, rhs, inverse_wide, face_map, transmissibility)
        return (state, jnp.mean(start, axis=1), jnp.mean(state, axis=1))
    ends, coarse_start, coarse_end = lax.map(propagate, start_states)
    coarse_op = coarse_map(partner, fracture_cond)
    high = lax.Precision.HIGHEST

    def advance(current, items):
        end_prev, mean_prev, mean_now, start_now = items
        fresh = end_prev + (current - mean_prev)[:, None, :]
        nxt = jnp.dot(coarse_op, current, precision=high) + (mean_now - jnp.dot(coarse_op, start_now, precision=high))
        return (nxt, fresh)
    items = (ends[:-1], coarse_end[:-1], coarse_end[1:], coarse_start[1:])
    last, fresh = lax.scan(advance, coarse_end[0], items)
    return jnp.concatenate([start_states[:1], fresh], axis=0)
```

```python
import functools

import jax
import jax.numpy as jnp
from jax import lax
from jax.experimental import pallas as pl
from jax.experimental.pallas import tpu as pltpu
from jax.sharding import PartitionSpec as P

F = 128
STEPS = 4
MESH = pl.DeviceIdType.MESH
f32, bf16 = jnp.float32, jnp.bfloat16
HI = lax.Precision.HIGHEST
PF, Q1, U2, Q3, MM, SR, MT = range(7)


def dot(a, b):
    return jnp.dot(a, b, preferred_element_type=f32)


def chosen(row):
    places = lax.broadcasted_iota(jnp.int32, (F, F), 0).astype(f32)
    hot = jnp.where(places == jnp.broadcast_to(row, (F, F)), 1.0, 0.0).astype(f32)
    return hot.T.astype(bf16)


def down_rows(row):
    return jnp.broadcast_to(row, (F, F)).T


def pick(hot, x):
    high = x.astype(bf16)
    low = (x - high.astype(f32)).astype(bf16)
    both = dot(hot, jnp.concatenate([high, low], axis=1))
    return both[:, :F] + both[:, F:]


def kernel(ns, nc, partner, cond, start_h, source_h, inv_h, fmap, trans, out,
           state, src, inv, rhs, v, sbuf, rbuf, smt, rmt, inn, gin, rg, tb, tg, hot, ghot,
           bp, xp, mp, prev, scoarse, rcoarse, hs, zb, zs, hb, gm, rm,
           lsem, ssem, rsem, esem, resem, csem, rcsem, hsem, rhsem, zsem, rzsem):
    c, s = lax.axis_index("cuts"), lax.axis_index("sub")
    width = state.shape[1]
    lo, hi = slice(0, F), slice(width - F, width)
    has_below, has_above = s > 0, s < ns - 1

    loads = [
        pltpu.make_async_copy(start_h.at[0], state, lsem.at[0]),
        pltpu.make_async_copy(source_h, src, lsem.at[1]),
        pltpu.make_async_copy(inv_h, inv, lsem.at[2]),
    ]
    for load in loads:
        load.start()

    hs[...] = jnp.zeros_like(hs)
    hb[...] = jnp.zeros_like(hb)
    rcoarse[...] = jnp.zeros_like(rcoarse)

    barrier = pltpu.get_barrier_semaphore()
    for o in range(1, ns):
        pl.semaphore_signal(barrier, inc=1, device_id={"sub": lax.rem(s + o, ns)}, device_id_type=MESH)
    for o in range(1, nc):
        pl.semaphore_signal(barrier, inc=1, device_id={"cuts": lax.rem(c + o, nc)}, device_id_type=MESH)

    def ext(d, i):
        to = lax.rem(s + 1, ns) if d == 0 else lax.rem(s + ns - 1, ns)
        if i == MT:
            a, b = smt.at[d], rmt.at[d]
        elif i == PF:
            a = state.at[1, pl.ds(width - F, F)] if d == 0 else state.at[0, pl.ds(0, F)]
            b = rbuf.at[d, i]
        else:
            a, b = sbuf.at[d, i], rbuf.at[d, i]
        return pltpu.make_async_remote_copy(
            src_ref=a, dst_ref=b, send_sem=ssem.at[d, i], recv_sem=rsem.at[d, i],
            device_id={"sub": to}, device_id_type=MESH)

    sends = (has_above, has_below)
    recvs = (has_below, has_above)

    def send(d, *which):
        @pl.when(sends[d])
        def _():
            for i in which:
                ext(d, i).start()

    def sent(*which):
        for d in (0, 1):
            @pl.when(sends[d])
            def _():
                for i in which:
                    ext(d, i).wait_send()

    def arrive(*which):
        for d in (0, 1):
            @pl.when(recvs[d])
            def _():
                for i in which:
                    ext(d, i).wait_recv()

    for d in (0, 1):
        @pl.when(jnp.logical_not(recvs[d]))
        def _():
            rbuf[d] = jnp.zeros(rbuf.shape[1:], f32)
            rmt[d] = jnp.zeros(rmt.shape[1:], f32)

    rows = [[fmap[b, pl.ds(k, 1), :].astype(f32) for k in (0, 1)] for b in (0, 1)]
    trow = [[trans[b, pl.ds(k, 1), :] for k in (0, 1)] for b in (0, 1)]
    for b in (0, 1):
        for k in (0, 1):
            tb[b, k] = down_rows(trow[b][k])
            hot[b, k] = chosen(rows[b][k])
    smt[...] = jnp.zeros_like(smt)
    smt[0, pl.ds(0, 1), :] = rows[1][1]
    smt[0, pl.ds(1, 1), :] = trow[1][1]
    smt[1, pl.ds(0, 1), :] = rows[0][0]
    smt[1, pl.ds(1, 1), :] = trow[0][0]

    loads[0].wait()
    @pl.when(c == 0)
    def _():
        prev[...] = state[...]
    scoarse[...] = jnp.zeros_like(scoarse)
    for b in (0, 1):
        scoarse[pl.ds(b, 1), :] = jnp.sum(state[b], axis=0, keepdims=True) / width

    pl.semaphore_wait(barrier, ns - 1 + nc - 1)

    for d in (0, 1):
        send(d, PF, MT)

    def coarse_back():
        return pltpu.make_async_remote_copy(
            src_ref=scoarse, dst_ref=rcoarse, send_sem=csem, recv_sem=rcsem,
            device_id={"cuts": lax.rem(c + nc - 1, nc)}, device_id_type=MESH)

    @pl.when(c > 0)
    def _():
        coarse_back().start()

    loads[1].wait()
    loads[2].wait()
    sbuf[0, MM] = inv[1, hi, hi].astype(f32)
    sbuf[1, MM] = inv[0, lo, lo].astype(f32)
    sbuf[0, SR] = src[1, hi].astype(f32)
    sbuf[1, SR] = src[0, lo].astype(f32)
    for d in (0, 1):
        send(d, MM, SR)

    bp[0] = dot(hot[1, 0], inv[0, hi, :]).astype(bf16)
    bp[1] = dot(hot[0, 1], inv[1, lo, :]).astype(bf16)
    inn[0] = pick(hot[1, 0], state[0, hi])
    inn[1] = pick(hot[0, 1], state[1, lo])

    def inner_faces():
        v[0, hi] = (rhs[0, hi] + tb[0, 1] * inn[1]).astype(bf16)
        v[1, lo] = (rhs[1, lo] + tb[1, 0] * inn[0]).astype(bf16)

    def inner_sweep():
        inn[0] = dot(bp[0], v[0])
        inn[1] = dot(bp[1], v[1])

    def outer_faces(below, above):
        v[0, lo] = (rhs[0, lo] + tb[0, 0] * below).astype(bf16)
        v[1, hi] = (rhs[1, hi] + tb[1, 1] * above).astype(bf16)

    def ghost(d):
        return dot(mp[d], (rg[d] + tg[d] * gin[d]).astype(bf16))

    npad = gm.shape[0]
    ri = lax.broadcasted_iota(jnp.int32, (npad, npad), 0)
    ci = lax.broadcasted_iota(jnp.int32, (npad, npad), 1)

    def coarse_inverse():
        def place(b):
            return 8 * lax.shift_right_logical(b, 1) + lax.bitwise_and(b, 1)

        def link(b, w):
            q = partner[b]
            at, to, g = place(b), place(q), cond[b]
            w = w + jnp.where((ri == at) & (ci == to), g, 0.0)
            return w + jnp.where((ri == to) & (ci == at), g, 0.0)

        real_r = lax.bitwise_and(ri, 7) < 2
        real_c = lax.bitwise_and(ci, 7) < 2
        br, bc = place_back(ri), place_back(ci)
        chain = jnp.where(real_r & real_c & ((br - bc == 1) | (bc - br == 1)), 1.0, 0.0).astype(f32)
        w = lax.fori_loop(0, 2 * ns, link, chain)
        total = jnp.sum(w, axis=1, keepdims=True)
        system = jnp.where(ri == ci, 1.0 + total, 0.0) - w

        def pivot(b, a):
            at = place(b)
            col = jnp.sum(jnp.where(ci == at, a, 0.0), axis=1, keepdims=True)
            row = jnp.sum(jnp.where(ri == at, a, 0.0), axis=0, keepdims=True)
            d = jnp.sum(jnp.where((ci == at) & (ri == at), a, 0.0), axis=(0, 1), keepdims=True)
            inv_d = 1.0 / d
            new = a - col * (row * inv_d)
            new = jnp.where(ri == at, row * inv_d, new)
            new = jnp.where(ci == at, col * inv_d, new)
            return jnp.where((ci == at) & (ri == at), -inv_d, new)

        gm[...] = -lax.fori_loop(0, 2 * ns, pivot, system)
        rm[...] = jnp.zeros_like(rm)

    def place_back(i):
        return 2 * lax.shift_right_logical(i, 3) + lax.bitwise_and(i, 7)

    rr = lax.broadcasted_iota(jnp.int32, rm.shape, 0)
    rc = lax.broadcasted_iota(jnp.int32, rm.shape, 1)

    def coarse_powers(first, count):
        def one(i, _):
            k = nc - 1 - first - i
            j = c - 1 - k
            unit = lax.bitwise_and(rr, 7)
            same = (unit < 2) & (unit == lax.bitwise_and(rc, 7))
            here = same & (rr - unit == 8 * s) & (rc - unit == 8 * j) & (k >= 1)
            rm[...] = jnp.dot(gm[...], rm[...] + jnp.where(here, 1.0, 0.0), precision=HI,
                              preferred_element_type=f32)
            return 0
        lax.fori_loop(0, count, one, 0)

    half = nc // 2

    def step(n, _):
        for b in (0, 1):
            r = state[b] + src[b].astype(f32)
            rhs[b] = r
            v[b] = r.astype(bf16)
        inner_faces()
        sbuf[0, Q1] = dot(inv[1, hi, 0:width - F], v[1, 0:width - F])
        send(0, Q1)
        sbuf[1, Q1] = dot(inv[0, lo, F:width], v[0, F:width])
        send(1, Q1)

        @pl.when(n == 1)
        def _():
            coarse_inverse()

        @pl.when(n == 2)
        def _():
            coarse_powers(half, nc - 1 - half)

        @pl.when(n == 0)
        def _():
            arrive(MT)
            for d in (0, 1):
                ghot[d] = chosen(rmt[d, pl.ds(0, 1), :])
                tg[d] = down_rows(rmt[d, pl.ds(1, 1), :])
            xp[0] = dot(ghot[0], inv[0, lo, :]).astype(bf16)
            xp[1] = dot(ghot[1], inv[1, hi, :]).astype(bf16)
            gin[0] = pick(ghot[0], state[0, lo])
            gin[1] = pick(ghot[1], state[1, hi])

        arrive(PF)
        outer_faces(pick(hot[0, 0], rbuf[0, PF]), pick(hot[1, 1], rbuf[1, PF]))
        inner_sweep()

        @pl.when(n == 0)
        def _():
            arrive(MM, SR)
            mp[0] = dot(hot[0, 0], rbuf[0, MM].astype(bf16)).astype(bf16)
            mp[1] = dot(hot[1, 1], rbuf[1, MM].astype(bf16)).astype(bf16)
            sent(MM, SR, MT)

        for d in (0, 1):
            rg[d] = rbuf[d, PF] + rbuf[d, SR]
        own = [ghost(d) for d in (0, 1)]
        arrive(Q1)
        below = pick(hot[0, 0], rbuf[0, Q1]) + own[0]
        above = pick(hot[1, 1], rbuf[1, Q1]) + own[1]
        sent(PF, Q1)

        outer_faces(below, above)
        inner_faces()
        up = dot(xp[1], v[1])
        sbuf[0, U2] = up
        gin[1] = up
        send(0, U2)
        down = dot(xp[0], v[0])
        sbuf[1, U2] = down
        gin[0] = down
        send(1, U2)
        inner_sweep()
        inner_faces()
        sbuf[0, Q3] = dot(xp[1, :, 0:width - F], v[1, 0:width - F])
        send(0, Q3)
        sbuf[1, Q3] = dot(xp[0, :, F:width], v[0, F:width])
        send(1, Q3)

        @pl.when(n == 1)
        def _():
            coarse_powers(0, half)

        own = [ghost(d) for d in (0, 1)]
        arrive(U2)
        outer_faces(rbuf[0, U2], rbuf[1, U2])
        inner_sweep()
        arrive(Q3)
        below = rbuf[0, Q3] + own[0]
        above = rbuf[1, Q3] + own[1]
        sent(U2, Q3)

        outer_faces(below, above)
        inner_faces()
        state[1, hi] = dot(inv[1, hi, :], v[1])
        state[0, lo] = dot(inv[0, lo, :], v[0])

        @pl.when(n < STEPS - 1)
        def _():
            send(0, PF)
            send(1, PF)

        state[0, F:width] = dot(inv[0, F:width, :], v[0])
        state[1, 0:width - F] = dot(inv[1, 0:width - F, :], v[1])

        @pl.when(n < STEPS - 1)
        def _():
            inner_sweep()
            gin[0] = dot(xp[0], v[0])
            gin[1] = dot(xp[1], v[1])
        return 0

    lax.fori_loop(0, STEPS, step, 0)

    def end(b):
        return pltpu.make_async_remote_copy(
            src_ref=state.at[b], dst_ref=prev.at[b], send_sem=esem.at[b], recv_sem=resem.at[b],
            device_id={"cuts": lax.rem(c + 1, nc)}, device_id_type=MESH)

    def jump(o):
        return pltpu.make_async_remote_copy(
            src_ref=hb, dst_ref=hs.at[c], send_sem=hsem.at[o], recv_sem=rhsem.at[c],
            device_id={"cuts": lax.rem(c + o, nc)}, device_id_type=MESH)

    def jump_from(o):
        at = lax.rem(c + nc - o, nc)
        return pltpu.make_async_remote_copy(
            src_ref=hb, dst_ref=hs.at[at], send_sem=hsem.at[o], recv_sem=rhsem.at[at],
            device_id={"cuts": at}, device_id_type=MESH)

    def part(o):
        to = lax.rem(s + o, ns)
        return pltpu.make_async_remote_copy(
            src_ref=zb.at[to], dst_ref=zs.at[s], send_sem=zsem.at[o], recv_sem=rzsem.at[s],
            device_id={"sub": to}, device_id_type=MESH)

    def part_from(o):
        at = lax.rem(s + ns - o, ns)
        return pltpu.make_async_remote_copy(
            src_ref=zb.at[at], dst_ref=zs.at[at], send_sem=zsem.at[o], recv_sem=rzsem.at[at],
            device_id={"sub": at}, device_id_type=MESH)

    @pl.when(c < nc - 1)
    def _():
        coarse_back().wait_recv()

    for b in (0, 1):
        hb[pl.ds(b, 1), :] = jnp.sum(state[b], axis=0, keepdims=True) / width - rcoarse[pl.ds(b, 1), :]
    for o in range(2, nc):
        @pl.when(c + o < nc)
        def _():
            jump(o).start()

    @pl.when(c < nc - 1)
    def _():
        for b in (0, 1):
            end(b).start()

    @pl.when(c > 0)
    def _():
        coarse_back().wait_send()

    for o in range(2, nc):
        @pl.when(c - o >= 0)
        def _():
            jump_from(o).wait_recv()

    z = jnp.dot(rm[...], hs[...].reshape(8 * nc, F), precision=HI, preferred_element_type=f32)
    zb[...] = z.reshape(ns, 8, F)
    for o in range(1, ns):
        part(o).start()
    for o in range(1, ns):
        part_from(o).wait_recv()
    zs[s] = zb[s]
    w = jnp.sum(zs[...], axis=0)

    @pl.when(c > 0)
    def _():
        for b in (0, 1):
            end(b).wait_recv()

    for b in (0, 1):
        out[0, b] = prev[b] + jnp.broadcast_to(w[b:b + 1], (width, F))

    for o in range(2, nc):
        @pl.when(c + o < nc)
        def _():
            jump(o).wait_send()
    for o in range(1, ns):
        part(o).wait_send()

    @pl.when(c < nc - 1)
    def _():
        for b in (0, 1):
            end(b).wait_send()


def solution(mesh):
    ns, nc = mesh.shape["sub"], mesh.shape["cuts"]

    def on_device(start, source, inverse, face_map, trans, partner, cond):
        width, cols = start.shape[2:]
        any_ = pl.BlockSpec(memory_space=pl.ANY)
        vmem = pl.BlockSpec(memory_space=pltpu.VMEM)
        smem = pl.BlockSpec(memory_space=pltpu.SMEM)
        V, S = pltpu.VMEM, pltpu.SemaphoreType.DMA
        scratch = dict(
            state=V((2, width, cols), f32), src=V((2, width, cols), bf16), inv=V((2, width, width), bf16),
            rhs=V((2, width, cols), f32), v=V((2, width, cols), bf16),
            sbuf=V((2, 6, F, cols), f32), rbuf=V((2, 6, F, cols), f32),
            smt=V((2, 8, F), f32), rmt=V((2, 8, F), f32),
            inn=V((2, F, cols), f32), gin=V((2, F, cols), f32), rg=V((2, F, cols), f32),
            tb=V((2, 2, F, cols), f32), tg=V((2, F, cols), f32),
            hot=V((2, 2, F, F), bf16), ghot=V((2, F, F), bf16),
            bp=V((2, F, width), bf16), xp=V((2, F, width), bf16), mp=V((2, F, F), bf16),
            prev=V((2, width, cols), f32), scoarse=V((8, cols), f32), rcoarse=V((8, cols), f32),
            hs=V((nc, 8, cols), f32), zb=V((ns, 8, cols), f32), zs=V((ns, 8, cols), f32),
            hb=V((8, cols), f32), gm=V((8 * ns, 8 * ns), f32), rm=V((8 * ns, 8 * nc), f32),
            lsem=S((3,)), ssem=S((2, 7)), rsem=S((2, 7)), esem=S((2,)), resem=S((2,)),
            csem=S(()), rcsem=S(()), hsem=S((nc,)), rhsem=S((nc,)), zsem=S((ns,)), rzsem=S((ns,)),
        )
        return pl.pallas_call(
            functools.partial(kernel, ns, nc),
            out_shape=jax.ShapeDtypeStruct(start.shape, f32),
            in_specs=[smem, smem, any_, any_, any_, vmem, vmem],
            out_specs=vmem,
            scratch_shapes=list(scratch.values()),
            compiler_params=pltpu.CompilerParams(collective_id=0, has_side_effects=True),
            name="parareal",
        )(partner, cond, start, source, inverse, face_map, trans)

    in_specs = (
        P("cuts", "sub", None, None),
        P("sub", None, None),
        P("sub", None, None),
        P("sub", None, None),
        P("sub", None, None),
        P(),
        P(),
    )
    return jax.shard_map(on_device, mesh=mesh, in_specs=in_specs,
                         out_specs=P("cuts", "sub", None, None), check_vma=False)
```

```python
import functools

import jax
import jax.numpy as jnp
from jax import lax
from jax.experimental import pallas as pl
from jax.experimental.pallas import tpu as pltpu
from jax.sharding import PartitionSpec as P

F = 128
STEPS = 4
MESH = pl.DeviceIdType.MESH
f32, bf16 = jnp.float32, jnp.bfloat16
HI = lax.Precision.HIGHEST
PF, Q1, U2, Q3, MT = range(5)


def dot(a, b):
    return jnp.dot(a, b, preferred_element_type=f32)


def chosen(row):
    places = lax.broadcasted_iota(jnp.int32, (F, F), 0).astype(f32)
    hot = jnp.where(places == jnp.broadcast_to(row, (F, F)), 1.0, 0.0).astype(f32)
    return hot.T.astype(bf16)


def down_rows(row):
    return jnp.broadcast_to(row, (F, F)).T


def pick(hot, x):
    high = x.astype(bf16)
    low = (x - high.astype(f32)).astype(bf16)
    both = dot(hot, jnp.concatenate([high, low], axis=1))
    return both[:, :F] + both[:, F:]


def kernel(ns, nc, partner, cond, start_h, source_h, inv_h, fmap, trans, prev, wout,
           state, src, inv, face, rf, vf, vi, cn, ci, bx, bi, sbuf, rbuf, smt, rmt, sst, rst,
           inn, gin, rg, tb, tg, hot, ghot, mp, scoarse, rcoarse, hs, zb, zs, hb, gm, rm, rw,
           lsem, ssem, rsem, psem, rpsem, fsem, rfsem, esem, resem, csem, rcsem, hsem, rhsem, zsem, rzsem):
    c, s = lax.axis_index("cuts"), lax.axis_index("sub")
    width = state.shape[1]
    L, U, I = slice(0, F), slice(width - F, width), slice(F, width - F)
    fL, fU = slice(0, F), slice(F, 2 * F)
    has_below, has_above = s > 0, s < ns - 1

    loads = [
        pltpu.make_async_copy(start_h.at[0], state, lsem.at[0]),
        pltpu.make_async_copy(source_h, src, lsem.at[1]),
        pltpu.make_async_copy(inv_h, inv, lsem.at[2]),
    ]
    for load in loads:
        load.start()

    hs[...] = jnp.zeros_like(hs)
    hb[...] = jnp.zeros_like(hb)
    rcoarse[...] = jnp.zeros_like(rcoarse)

    barrier = pltpu.get_barrier_semaphore()
    for o in range(1, ns):
        pl.semaphore_signal(barrier, inc=1, device_id={"sub": lax.rem(s + o, ns)}, device_id_type=MESH)
    for o in range(1, nc):
        pl.semaphore_signal(barrier, inc=1, device_id={"cuts": lax.rem(c + o, nc)}, device_id_type=MESH)

    def towards(d):
        return lax.rem(s + 1, ns) if d == 0 else lax.rem(s + ns - 1, ns)

    def ext(d, i):
        if i == MT:
            a, b = smt.at[d], rmt.at[d]
        elif i == PF:
            a = state.at[1, pl.ds(width - F, F)] if d == 0 else state.at[0, pl.ds(0, F)]
            b = rbuf.at[d, i]
        else:
            a, b = sbuf.at[d, i], rbuf.at[d, i]
        return pltpu.make_async_remote_copy(
            src_ref=a, dst_ref=b, send_sem=ssem.at[d, i], recv_sem=rsem.at[d, i],
            device_id={"sub": towards(d)}, device_id_type=MESH)

    sends = (has_above, has_below)
    recvs = (has_below, has_above)

    def send(d, *which):
        @pl.when(sends[d])
        def _():
            for i in which:
                ext(d, i).start()

    def sent(*which):
        for d in (0, 1):
            @pl.when(sends[d])
            def _():
                for i in which:
                    ext(d, i).wait_send()

    def arrive(*which):
        for d in (0, 1):
            @pl.when(recvs[d])
            def _():
                for i in which:
                    ext(d, i).wait_recv()

    group = min(8, nc)
    size = F // group
    own = lax.rem(c, group)

    def piece(ref, d, at):
        return ref.at[d, :, pl.ds(pl.multiple_of(at * size, size), size)]

    def across(d):
        return pltpu.make_async_remote_copy(
            src_ref=piece(sst, d, own), dst_ref=piece(rst, d, own), send_sem=psem.at[d], recv_sem=rpsem.at[d],
            device_id={"sub": towards(d)}, device_id_type=MESH)

    def along(d, o):
        return pltpu.make_async_remote_copy(
            src_ref=piece(rst, d, own), dst_ref=piece(rst, d, own), send_sem=fsem.at[d, o],
            recv_sem=rfsem.at[d, own], device_id={"cuts": c - own + lax.rem(own + o, group)}, device_id_type=MESH)

    def along_from(d, o):
        at = lax.rem(own + group - o, group)
        return pltpu.make_async_remote_copy(
            src_ref=piece(rst, d, at), dst_ref=piece(rst, d, at), send_sem=fsem.at[d, o],
            recv_sem=rfsem.at[d, at], device_id={"cuts": c - own + at}, device_id_type=MESH)

    for d in (0, 1):
        @pl.when(jnp.logical_not(recvs[d]))
        def _():
            rbuf[d] = jnp.zeros(rbuf.shape[1:], f32)
            rmt[d] = jnp.zeros(rmt.shape[1:], f32)
            rst[d] = jnp.zeros(rst.shape[1:], f32)

    rows = [[fmap[b, pl.ds(k, 1), :].astype(f32) for k in (0, 1)] for b in (0, 1)]
    trow = [[trans[b, pl.ds(k, 1), :] for k in (0, 1)] for b in (0, 1)]
    smt[...] = jnp.zeros_like(smt)
    smt[0, pl.ds(0, 1), :] = rows[1][1]
    smt[0, pl.ds(1, 1), :] = trow[1][1]
    smt[1, pl.ds(0, 1), :] = rows[0][0]
    smt[1, pl.ds(1, 1), :] = trow[0][0]
    for b in (0, 1):
        for k in (0, 1):
            tb[b, k] = down_rows(trow[b][k])
            hot[b, k] = chosen(rows[b][k])

    loads[0].wait()
    keep = pltpu.make_async_copy(state, prev, lsem.at[3])

    @pl.when(c == 0)
    def _():
        keep.start()

    loads[1].wait()
    sst[0, 1] = src[1, U].astype(f32)
    sst[1, 1] = src[0, L].astype(f32)
    loads[2].wait()
    sst[0, 0] = inv[1, U, U].astype(f32)
    sst[1, 0] = inv[0, L, L].astype(f32)

    pl.semaphore_wait(barrier, ns - 1 + nc - 1)

    for d in (0, 1):
        send(d, MT, PF)

        @pl.when(sends[d])
        def _():
            across(d).start()

    def own_rows(b):
        rows_of = dot(hot[1, 0], inv[0, U, :]) if b == 0 else dot(hot[0, 1], inv[1, L, :])
        rows_of = rows_of.astype(bf16)
        bx[b, F:, fL] = rows_of[:, L]
        bx[b, F:, fU] = rows_of[:, U]
        bi[b, F:] = rows_of[:, I]

    inn[0] = pick(hot[1, 0], state[0, U])
    inn[1] = pick(hot[0, 1], state[1, L])

    def inner_faces():
        vf[0, fU] = (rf[0, fU] + tb[0, 1] * inn[1]).astype(bf16)
        vf[1, fL] = (rf[1, fL] + tb[1, 0] * inn[0]).astype(bf16)

    def inner_sweep():
        for b in (0, 1):
            inn[b] = ci[b, F:] + dot(bx[b, F:], vf[b])

    def outer_faces(below, above):
        vf[0, fL] = (rf[0, fL] + tb[0, 0] * below).astype(bf16)
        vf[1, fU] = (rf[1, fU] + tb[1, 1] * above).astype(bf16)

    def ghost(d):
        return dot(mp[d], (rg[d] + tg[d] * gin[d]).astype(bf16))

    count = 2 * ns
    ri = lax.broadcasted_iota(jnp.int32, (count, count), 0)
    ki = lax.broadcasted_iota(jnp.int32, (count, count), 1)
    pieces = -(-(nc - 1) // 3)

    def coarse_piece(w):
        @pl.when(w == 1)
        def _():
            def link(b, a):
                q, g = partner[b], cond[b]
                a = a + jnp.where((ri == b) & (ki == q), g, 0.0)
                return a + jnp.where((ri == q) & (ki == b), g, 0.0)

            chain = jnp.where((ri - ki == 1) | (ki - ri == 1), 1.0, 0.0).astype(f32)
            a = lax.fori_loop(0, count, link, chain)
            gm[...] = jnp.where(ri == ki, 1.0 + jnp.sum(a, axis=1, keepdims=True), 0.0) - a

        @pl.when((w >= 1) & (w <= 4))
        def _():
            def pivot(i, a):
                at = (w - 1) * (count // 4) + i
                col = jnp.sum(jnp.where(ki == at, a, 0.0), axis=1, keepdims=True)
                row = jnp.sum(jnp.where(ri == at, a, 0.0), axis=0, keepdims=True)
                d = jnp.sum(jnp.where(ki[:1] == at, row, 0.0), axis=1, keepdims=True)
                inv_d = 1.0 / d
                scaled = row * inv_d
                new = jnp.where(ri == at, scaled, a - col * scaled)
                new = jnp.where(ki == at, col * inv_d, new)
                return jnp.where((ki == at) & (ri == at), -inv_d, new)

            gm[...] = lax.fori_loop(0, count // 4, pivot, gm[...])

        @pl.when(w == 5)
        def _():
            rw[...] = jnp.zeros_like(rw)

        @pl.when(w >= 5)
        def _():
            rr = lax.broadcasted_iota(jnp.int32, rw.shape, 0)
            unit = lax.bitwise_and(lax.broadcasted_iota(jnp.int32, rw.shape, 1), 7)
            slot = lax.shift_right_logical(lax.broadcasted_iota(jnp.int32, rw.shape, 1), 3)

            def power(i, acc):
                k = (8 - w) * pieces - i
                here = (unit < 2) & (rr - unit == 2 * s) & (slot == c - 1 - k)
                return -jnp.dot(gm[...], acc + jnp.where(here, 1.0, 0.0), precision=HI,
                                preferred_element_type=f32)

            rw[...] = lax.fori_loop(0, pieces, power, rw[...])

        @pl.when(w == 7)
        def _():
            pr = lax.broadcasted_iota(jnp.int32, (8 * ns, count), 0)
            pc = lax.broadcasted_iota(jnp.int32, (8 * ns, count), 1)
            half = lax.bitwise_and(pr, 7)
            spread = jnp.where((half < 2) & (2 * lax.shift_right_logical(pr, 3) + half == pc), 1.0, 0.0)
            rm[...] = jnp.dot(spread.astype(f32), rw[...], precision=HI, preferred_element_type=f32)

    def step(n, _):
        for b in (0, 1):
            vi[b] = (state[b, I] + src[b, I].astype(f32)).astype(bf16)
            rf[b, fL] = state[b, L] + src[b, L].astype(f32)
            rf[b, fU] = state[b, U] + src[b, U].astype(f32)
        inner_faces()
        cn[1, U] = dot(inv[1, U, I], vi[1])
        sbuf[0, Q1] = cn[1, U] + dot(inv[1, U, L], vf[1, fL])
        send(0, Q1)
        cn[0, L] = dot(inv[0, L, I], vi[0])
        sbuf[1, Q1] = cn[0, L] + dot(inv[0, L, U], vf[0, fU])
        send(1, Q1)

        @pl.when(n == 0)
        def _():
            scoarse[...] = jnp.zeros_like(scoarse)
            for b in (0, 1):
                scoarse[pl.ds(b, 1), :] = jnp.sum(state[b], axis=0, keepdims=True) / width
                own_rows(b)
                face[b, :, fL] = inv[b, :, L]
                face[b, :, fU] = inv[b, :, U]

            @pl.when(c > 0)
            def _():
                coarse_back().start()
            arrive(MT)
            for d in (0, 1):
                ghot[d] = chosen(rmt[d, pl.ds(0, 1), :])
                tg[d] = down_rows(rmt[d, pl.ds(1, 1), :])
            for b in (0, 1):
                read = dot(ghot[b], inv[0, L, :] if b == 0 else inv[1, U, :]).astype(bf16)
                bx[b, :F, fL] = read[:, L]
                bx[b, :F, fU] = read[:, U]
                bi[b, :F] = read[:, I]
            gin[0] = pick(ghot[0], state[0, L])
            gin[1] = pick(ghot[1], state[1, U])
            for d in (0, 1):
                @pl.when(recvs[d])
                def _():
                    across(d).wait_recv()
                    for o in range(1, group):
                        along(d, o).start()

        for b in (0, 1):
            ci[b] = dot(bi[b], vi[b])
        cn[0, F:] = dot(inv[0, F:, I], vi[0])
        cn[1, :width - F] = dot(inv[1, :width - F, I], vi[1])
        coarse_piece(2 * n)

        arrive(PF)
        outer_faces(pick(hot[0, 0], rbuf[0, PF]), pick(hot[1, 1], rbuf[1, PF]))
        inner_sweep()

        @pl.when(n == 0)
        def _():
            for d in (0, 1):
                @pl.when(sends[d])
                def _():
                    across(d).wait_send()

                @pl.when(recvs[d])
                def _():
                    for o in range(1, group):
                        along_from(d, o).wait_recv()
                    for o in range(1, group):
                        along(d, o).wait_send()
            mp[0] = dot(hot[0, 0], rst[0, 0].astype(bf16)).astype(bf16)
            mp[1] = dot(hot[1, 1], rst[1, 0].astype(bf16)).astype(bf16)
            sent(MT)

            @pl.when(c == 0)
            def _():
                keep.wait()

        for d in (0, 1):
            rg[d] = rbuf[d, PF] + rst[d, 1]
        more = [ghost(d) for d in (0, 1)]
        arrive(Q1)
        below = pick(hot[0, 0], rbuf[0, Q1]) + more[0]
        above = pick(hot[1, 1], rbuf[1, Q1]) + more[1]
        sent(PF, Q1)

        outer_faces(below, above)
        inner_faces()
        for b in (1, 0):
            y = ci[b] + dot(bx[b], vf[b])
            sbuf[1 - b, U2] = y[:F]
            gin[b] = y[:F]
            inn[b] = y[F:]
            send(1 - b, U2)
        inner_faces()
        sbuf[0, Q3] = ci[1, :F] + dot(bx[1, :F, fL], vf[1, fL])
        send(0, Q3)
        sbuf[1, Q3] = ci[0, :F] + dot(bx[0, :F, fU], vf[0, fU])
        send(1, Q3)
        coarse_piece(2 * n + 1)

        more = [ghost(d) for d in (0, 1)]
        arrive(U2)
        outer_faces(rbuf[0, U2], rbuf[1, U2])
        inner_sweep()
        arrive(Q3)
        below = rbuf[0, Q3] + more[0]
        above = rbuf[1, Q3] + more[1]
        sent(U2, Q3)

        outer_faces(below, above)
        inner_faces()
        state[1, U] = cn[1, U] + dot(face[1, U], vf[1])
        state[0, L] = cn[0, L] + dot(face[0, L], vf[0])

        @pl.when(n < STEPS - 1)
        def _():
            send(0, PF)
            send(1, PF)

        state[1, :width - F] = cn[1, :width - F] + dot(face[1, :width - F], vf[1])
        state[0, F:] = cn[0, F:] + dot(face[0, F:], vf[0])

        @pl.when(n < STEPS - 1)
        def _():
            for b in (0, 1):
                y = ci[b] + dot(bx[b], vf[b])
                gin[b] = y[:F]
                inn[b] = y[F:]
        return 0

    def coarse_back():
        return pltpu.make_async_remote_copy(
            src_ref=scoarse, dst_ref=rcoarse, send_sem=csem, recv_sem=rcsem,
            device_id={"cuts": lax.rem(c + nc - 1, nc)}, device_id_type=MESH)

    lax.fori_loop(0, STEPS, step, 0)

    def end(b):
        return pltpu.make_async_remote_copy(
            src_ref=state.at[b], dst_ref=prev.at[b], send_sem=esem.at[b], recv_sem=resem.at[b],
            device_id={"cuts": lax.rem(c + 1, nc)}, device_id_type=MESH)

    def jump(o):
        return pltpu.make_async_remote_copy(
            src_ref=hb, dst_ref=hs.at[c], send_sem=hsem.at[o], recv_sem=rhsem.at[c],
            device_id={"cuts": lax.rem(c + o, nc)}, device_id_type=MESH)

    def jump_from(o):
        at = lax.rem(c + nc - o, nc)
        return pltpu.make_async_remote_copy(
            src_ref=hb, dst_ref=hs.at[at], send_sem=hsem.at[o], recv_sem=rhsem.at[at],
            device_id={"cuts": at}, device_id_type=MESH)

    def part(o):
        to = lax.rem(s + o, ns)
        return pltpu.make_async_remote_copy(
            src_ref=zb.at[to], dst_ref=zs.at[s], send_sem=zsem.at[o], recv_sem=rzsem.at[s],
            device_id={"sub": to}, device_id_type=MESH)

    def part_from(o):
        at = lax.rem(s + ns - o, ns)
        return pltpu.make_async_remote_copy(
            src_ref=zb.at[at], dst_ref=zs.at[at], send_sem=zsem.at[o], recv_sem=rzsem.at[at],
            device_id={"sub": at}, device_id_type=MESH)

    @pl.when(c < nc - 1)
    def _():
        coarse_back().wait_recv()

    for b in (0, 1):
        hb[pl.ds(b, 1), :] = jnp.sum(state[b], axis=0, keepdims=True) / width - rcoarse[pl.ds(b, 1), :]
    for o in range(2, nc):
        @pl.when(c + o < nc)
        def _():
            jump(o).start()

    @pl.when(c < nc - 1)
    def _():
        for b in (0, 1):
            end(b).start()

    @pl.when(c > 0)
    def _():
        coarse_back().wait_send()

    for o in range(2, nc):
        @pl.when(c - o >= 0)
        def _():
            jump_from(o).wait_recv()

    z = jnp.dot(rm[...], hs[...].reshape(8 * nc, F), precision=HI, preferred_element_type=f32)
    zb[...] = z.reshape(ns, 8, F)
    for o in range(1, ns):
        part(o).start()
    for o in range(1, ns):
        part_from(o).wait_recv()
    zs[s] = zb[s]
    wout[...] = jnp.sum(zs[...], axis=0)[:2]

    @pl.when(c > 0)
    def _():
        for b in (0, 1):
            end(b).wait_recv()

    for o in range(2, nc):
        @pl.when(c + o < nc)
        def _():
            jump(o).wait_send()
    for o in range(1, ns):
        part(o).wait_send()

    @pl.when(c < nc - 1)
    def _():
        for b in (0, 1):
            end(b).wait_send()


def solution(mesh):
    ns, nc = mesh.shape["sub"], mesh.shape["cuts"]

    def on_device(start, source, inverse, face_map, trans, partner, cond):
        width, cols = start.shape[2:]
        any_ = pl.BlockSpec(memory_space=pl.ANY)
        vmem = pl.BlockSpec(memory_space=pltpu.VMEM)
        smem = pl.BlockSpec(memory_space=pltpu.SMEM)
        V, S = pltpu.VMEM, pltpu.SemaphoreType.DMA
        scratch = dict(
            state=V((2, width, cols), f32), src=V((2, width, cols), bf16), inv=V((2, width, width), bf16),
            face=V((2, width, 2 * F), bf16), rf=V((2, 2 * F, cols), f32), vf=V((2, 2 * F, cols), bf16),
            vi=V((2, width - 2 * F, cols), bf16), cn=V((2, width, cols), f32), ci=V((2, 2 * F, cols), f32),
            bx=V((2, 2 * F, 2 * F), bf16), bi=V((2, 2 * F, width - 2 * F), bf16),
            sbuf=V((2, 4, F, cols), f32), rbuf=V((2, 4, F, cols), f32),
            smt=V((2, 8, F), f32), rmt=V((2, 8, F), f32), sst=V((2, 2, F, cols), f32), rst=V((2, 2, F, cols), f32),
            inn=V((2, F, cols), f32), gin=V((2, F, cols), f32), rg=V((2, F, cols), f32),
            tb=V((2, 2, F, cols), f32), tg=V((2, F, cols), f32),
            hot=V((2, 2, F, F), bf16), ghot=V((2, F, F), bf16), mp=V((2, F, F), bf16),
            scoarse=V((8, cols), f32), rcoarse=V((8, cols), f32),
            hs=V((nc, 8, cols), f32), zb=V((ns, 8, cols), f32), zs=V((ns, 8, cols), f32),
            hb=V((8, cols), f32), gm=V((2 * ns, 2 * ns), f32), rm=V((8 * ns, 8 * nc), f32),
            rw=V((2 * ns, 8 * nc), f32),
            lsem=S((4,)), ssem=S((2, 5)), rsem=S((2, 5)), psem=S((2,)), rpsem=S((2,)),
            fsem=S((2, 8)), rfsem=S((2, 8)), esem=S((2,)), resem=S((2,)),
            csem=S(()), rcsem=S(()), hsem=S((nc,)), rhsem=S((nc,)), zsem=S((ns,)), rzsem=S((ns,)),
        )
        ends, added = pl.pallas_call(
            functools.partial(kernel, ns, nc),
            out_shape=(jax.ShapeDtypeStruct(start.shape[1:], f32), jax.ShapeDtypeStruct((2, cols), f32)),
            in_specs=[smem, smem, any_, any_, any_, vmem, vmem],
            out_specs=(any_, vmem),
            scratch_shapes=list(scratch.values()),
            compiler_params=pltpu.CompilerParams(collective_id=0, has_side_effects=True),
            name="parareal",
        )(partner, cond, start, source, inverse, face_map, trans)
        return (ends + added[:, None, :])[None]

    in_specs = (
        P("cuts", "sub", None, None),
        P("sub", None, None),
        P("sub", None, None),
        P("sub", None, None),
        P("sub", None, None),
        P(),
        P(),
    )
    return jax.shard_map(on_device, mesh=mesh, in_specs=in_specs,
                         out_specs=P("cuts", "sub", None, None), check_vma=False)
```

```python
import functools

import jax
import jax.numpy as jnp
from jax import lax
from jax.experimental import pallas as pl
from jax.experimental.pallas import tpu as pltpu
from jax.sharding import PartitionSpec as P

F = 128
STEPS = 4
MESH = pl.DeviceIdType.MESH
f32, bf16 = jnp.float32, jnp.bfloat16
HI = lax.Precision.HIGHEST
PF, Q1, U2, Q3, MT = range(5)


def dot(a, b):
    return jnp.dot(a, b, preferred_element_type=f32)


def chosen(row):
    places = lax.broadcasted_iota(jnp.int32, (F, F), 0).astype(f32)
    hot = jnp.where(places == jnp.broadcast_to(row, (F, F)), 1.0, 0.0).astype(f32)
    return hot.T.astype(bf16)


def down_rows(row):
    return jnp.broadcast_to(row, (F, F)).T


def pick(hot, x):
    high = x.astype(bf16)
    low = (x - high.astype(f32)).astype(bf16)
    both = dot(hot, jnp.concatenate([high, low], axis=1))
    return both[:, :F] + both[:, F:]


def kernel(ns, nc, partner_h, cond_h, start_h, source_h, inv_h, fmap_h, trans_h, prev,
           partner, cond, fmap, trans,
           state, src, inv, face, rf, vf, vi, cn, ci, bx, bi, sbuf, rbuf, smt, rmt, sst, rst,
           inn, gin, rg, tb, tg, hot, ghot, mp, scoarse, rcoarse, hs, zb, zs, hb, gm, rm, rw,
           lsem, ssem, rsem, psem, rpsem, fsem, rfsem, esem, resem, csem, rcsem, hsem, rhsem, zsem, rzsem):
    c, s = lax.axis_index("cuts"), lax.axis_index("sub")
    width = state.shape[1]
    L, U, I = slice(0, F), slice(width - F, width), slice(F, width - F)
    fL, fU = slice(0, F), slice(F, 2 * F)
    has_below, has_above = s > 0, s < ns - 1

    loads = [
        pltpu.make_async_copy(start_h.at[0], state, lsem.at[0]),
        pltpu.make_async_copy(source_h, src, lsem.at[1]),
        pltpu.make_async_copy(inv_h, inv, lsem.at[2]),
        pltpu.make_async_copy(fmap_h, fmap, lsem.at[4]),
        pltpu.make_async_copy(trans_h, trans, lsem.at[5]),
        pltpu.make_async_copy(partner_h, partner, lsem.at[6]),
        pltpu.make_async_copy(cond_h, cond, lsem.at[7]),
    ]
    for k in (3, 4, 0, 1, 2, 5, 6):
        loads[k].start()

    hs[...] = jnp.zeros_like(hs)
    hb[...] = jnp.zeros_like(hb)
    rcoarse[...] = jnp.zeros_like(rcoarse)

    barrier = pltpu.get_barrier_semaphore()
    for o in range(1, ns):
        pl.semaphore_signal(barrier, inc=1, device_id={"sub": lax.rem(s + o, ns)}, device_id_type=MESH)
    for o in range(1, nc):
        pl.semaphore_signal(barrier, inc=1, device_id={"cuts": lax.rem(c + o, nc)}, device_id_type=MESH)

    def towards(d):
        return lax.rem(s + 1, ns) if d == 0 else lax.rem(s + ns - 1, ns)

    def ext(d, i):
        if i == MT:
            a, b = smt.at[d], rmt.at[d]
        elif i == PF:
            a = state.at[1, pl.ds(width - F, F)] if d == 0 else state.at[0, pl.ds(0, F)]
            b = rbuf.at[d, i]
        else:
            a, b = sbuf.at[d, i], rbuf.at[d, i]
        return pltpu.make_async_remote_copy(
            src_ref=a, dst_ref=b, send_sem=ssem.at[d, i], recv_sem=rsem.at[d, i],
            device_id={"sub": towards(d)}, device_id_type=MESH)

    sends = (has_above, has_below)
    recvs = (has_below, has_above)

    def send(d, *which):
        @pl.when(sends[d])
        def _():
            for i in which:
                ext(d, i).start()

    def sent(*which):
        for d in (0, 1):
            @pl.when(sends[d])
            def _():
                for i in which:
                    ext(d, i).wait_send()

    def arrive(*which):
        for d in (0, 1):
            @pl.when(recvs[d])
            def _():
                for i in which:
                    ext(d, i).wait_recv()

    group = min(8, nc)
    size = F // group
    own = lax.rem(c, group)

    def piece(ref, d, at):
        return ref.at[d, :, pl.ds(pl.multiple_of(at * size, size), size)]

    def across(d):
        return pltpu.make_async_remote_copy(
            src_ref=piece(sst, d, own), dst_ref=piece(rst, d, own), send_sem=psem.at[d], recv_sem=rpsem.at[d],
            device_id={"sub": towards(d)}, device_id_type=MESH)

    def along(d, o):
        return pltpu.make_async_remote_copy(
            src_ref=piece(rst, d, own), dst_ref=piece(rst, d, own), send_sem=fsem.at[d, o],
            recv_sem=rfsem.at[d, own], device_id={"cuts": c - own + lax.rem(own + o, group)}, device_id_type=MESH)

    def along_from(d, o):
        at = lax.rem(own + group - o, group)
        return pltpu.make_async_remote_copy(
            src_ref=piece(rst, d, at), dst_ref=piece(rst, d, at), send_sem=fsem.at[d, o],
            recv_sem=rfsem.at[d, at], device_id={"cuts": c - own + at}, device_id_type=MESH)

    for d in (0, 1):
        @pl.when(jnp.logical_not(recvs[d]))
        def _():
            rbuf[d] = jnp.zeros(rbuf.shape[1:], f32)
            rmt[d] = jnp.zeros(rmt.shape[1:], f32)
            rst[d] = jnp.zeros(rst.shape[1:], f32)

    loads[3].wait()
    loads[4].wait()
    rows = [[fmap[b, pl.ds(k, 1), :].astype(f32) for k in (0, 1)] for b in (0, 1)]
    trow = [[trans[b, pl.ds(k, 1), :] for k in (0, 1)] for b in (0, 1)]
    smt[...] = jnp.zeros_like(smt)
    smt[0, pl.ds(0, 1), :] = rows[1][1]
    smt[0, pl.ds(1, 1), :] = trow[1][1]
    smt[1, pl.ds(0, 1), :] = rows[0][0]
    smt[1, pl.ds(1, 1), :] = trow[0][0]
    for b in (0, 1):
        for k in (0, 1):
            tb[b, k] = down_rows(trow[b][k])
            hot[b, k] = chosen(rows[b][k])

    loads[0].wait()
    keep = pltpu.make_async_copy(start_h.at[0], prev.at[0], lsem.at[3])

    @pl.when(c == 0)
    def _():
        keep.start()

    loads[1].wait()
    sst[0, 1] = src[1, U].astype(f32)
    sst[1, 1] = src[0, L].astype(f32)
    loads[2].wait()
    sst[0, 0] = inv[1, U, U].astype(f32)
    sst[1, 0] = inv[0, L, L].astype(f32)

    pl.semaphore_wait(barrier, ns - 1 + nc - 1)

    for d in (0, 1):
        @pl.when(sends[d])
        def _():
            across(d).start()

        send(d, MT, PF)

    def own_rows(b):
        rows_of = dot(hot[1, 0], inv[0, U, :]) if b == 0 else dot(hot[0, 1], inv[1, L, :])
        rows_of = rows_of.astype(bf16)
        bx[b, F:, fL] = rows_of[:, L]
        bx[b, F:, fU] = rows_of[:, U]
        bi[b, F:] = rows_of[:, I]

    inn[0] = pick(hot[1, 0], state[0, U])
    inn[1] = pick(hot[0, 1], state[1, L])

    def inner_faces():
        vf[0, fU] = (rf[0, fU] + tb[0, 1] * inn[1]).astype(bf16)
        vf[1, fL] = (rf[1, fL] + tb[1, 0] * inn[0]).astype(bf16)

    def inner_sweep():
        for b in (0, 1):
            inn[b] = ci[b, F:] + dot(bx[b, F:], vf[b])

    def outer_faces(below, above):
        vf[0, fL] = (rf[0, fL] + tb[0, 0] * below).astype(bf16)
        vf[1, fU] = (rf[1, fU] + tb[1, 1] * above).astype(bf16)

    def ghost(d):
        return dot(mp[d], (rg[d] + tg[d] * gin[d]).astype(bf16))

    count = 2 * ns
    ri = lax.broadcasted_iota(jnp.int32, (count, count), 0)
    ki = lax.broadcasted_iota(jnp.int32, (count, count), 1)
    pieces = -(-(nc - 1) // 3)

    def coarse_piece(w):
        @pl.when(w == 1)
        def _():
            def link(b, a):
                q, g = partner[b], cond[b]
                a = a + jnp.where((ri == b) & (ki == q), g, 0.0)
                return a + jnp.where((ri == q) & (ki == b), g, 0.0)

            chain = jnp.where((ri - ki == 1) | (ki - ri == 1), 1.0, 0.0).astype(f32)
            a = lax.fori_loop(0, count, link, chain)
            gm[...] = jnp.where(ri == ki, 1.0 + jnp.sum(a, axis=1, keepdims=True), 0.0) - a

        @pl.when((w >= 1) & (w <= 4))
        def _():
            def pivot(i, a):
                at = (w - 1) * (count // 4) + i
                col = jnp.sum(jnp.where(ki == at, a, 0.0), axis=1, keepdims=True)
                row = jnp.sum(jnp.where(ri == at, a, 0.0), axis=0, keepdims=True)
                d = jnp.sum(jnp.where(ki[:1] == at, row, 0.0), axis=1, keepdims=True)
                inv_d = 1.0 / d
                scaled = row * inv_d
                new = jnp.where(ri == at, scaled, a - col * scaled)
                new = jnp.where(ki == at, col * inv_d, new)
                return jnp.where((ki == at) & (ri == at), -inv_d, new)

            gm[...] = lax.fori_loop(0, count // 4, pivot, gm[...])

        @pl.when(w == 5)
        def _():
            rw[...] = jnp.zeros_like(rw)

        @pl.when(w >= 5)
        def _():
            rr = lax.broadcasted_iota(jnp.int32, rw.shape, 0)
            unit = lax.bitwise_and(lax.broadcasted_iota(jnp.int32, rw.shape, 1), 7)
            slot = lax.shift_right_logical(lax.broadcasted_iota(jnp.int32, rw.shape, 1), 3)

            def power(i, acc):
                k = (8 - w) * pieces - i
                here = (unit < 2) & (rr - unit == 2 * s) & (slot == c - 1 - k)
                return -jnp.dot(gm[...], acc + jnp.where(here, 1.0, 0.0), precision=HI,
                                preferred_element_type=f32)

            rw[...] = lax.fori_loop(0, pieces, power, rw[...])

        @pl.when(w == 7)
        def _():
            pr = lax.broadcasted_iota(jnp.int32, (8 * ns, count), 0)
            pc = lax.broadcasted_iota(jnp.int32, (8 * ns, count), 1)
            half = lax.bitwise_and(pr, 7)
            spread = jnp.where((half < 2) & (2 * lax.shift_right_logical(pr, 3) + half == pc), 1.0, 0.0)
            rm[...] = jnp.dot(spread.astype(f32), rw[...], precision=HI, preferred_element_type=f32)

    def step(n, _):
        for b in (0, 1):
            vi[b] = (state[b, I] + src[b, I].astype(f32)).astype(bf16)
            rf[b, fL] = state[b, L] + src[b, L].astype(f32)
            rf[b, fU] = state[b, U] + src[b, U].astype(f32)
        inner_faces()
        cn[1, U] = dot(inv[1, U, I], vi[1])
        sbuf[0, Q1] = cn[1, U] + dot(inv[1, U, L], vf[1, fL])
        send(0, Q1)
        cn[0, L] = dot(inv[0, L, I], vi[0])
        sbuf[1, Q1] = cn[0, L] + dot(inv[0, L, U], vf[0, fU])
        send(1, Q1)

        @pl.when(n == 0)
        def _():
            scoarse[...] = jnp.zeros_like(scoarse)
            for b in (0, 1):
                scoarse[pl.ds(b, 1), :] = jnp.sum(state[b], axis=0, keepdims=True) / width
                own_rows(b)
                face[b, :, fL] = inv[b, :, L]
                face[b, :, fU] = inv[b, :, U]

            @pl.when(c > 0)
            def _():
                coarse_back().start()
            arrive(MT)
            for d in (0, 1):
                ghot[d] = chosen(rmt[d, pl.ds(0, 1), :])
                tg[d] = down_rows(rmt[d, pl.ds(1, 1), :])
            for b in (0, 1):
                read = dot(ghot[b], inv[0, L, :] if b == 0 else inv[1, U, :]).astype(bf16)
                bx[b, :F, fL] = read[:, L]
                bx[b, :F, fU] = read[:, U]
                bi[b, :F] = read[:, I]
            gin[0] = pick(ghot[0], state[0, L])
            gin[1] = pick(ghot[1], state[1, U])
            for d in (0, 1):
                @pl.when(recvs[d])
                def _():
                    across(d).wait_recv()
                    for o in range(1, group):
                        along(d, o).start()

        for b in (0, 1):
            ci[b] = dot(bi[b], vi[b])
        cn[0, F:] = dot(inv[0, F:, I], vi[0])
        cn[1, :width - F] = dot(inv[1, :width - F, I], vi[1])
        coarse_piece(2 * n)

        arrive(PF)
        outer_faces(pick(hot[0, 0], rbuf[0, PF]), pick(hot[1, 1], rbuf[1, PF]))
        inner_sweep()

        @pl.when(n == 0)
        def _():
            for d in (0, 1):
                @pl.when(sends[d])
                def _():
                    across(d).wait_send()

                @pl.when(recvs[d])
                def _():
                    for o in range(1, group):
                        along_from(d, o).wait_recv()
                    for o in range(1, group):
                        along(d, o).wait_send()
            mp[0] = dot(hot[0, 0], rst[0, 0].astype(bf16)).astype(bf16)
            mp[1] = dot(hot[1, 1], rst[1, 0].astype(bf16)).astype(bf16)
            sent(MT)

            loads[5].wait()
            loads[6].wait()

        for d in (0, 1):
            rg[d] = rbuf[d, PF] + rst[d, 1]
        more = [ghost(d) for d in (0, 1)]
        arrive(Q1)
        below = pick(hot[0, 0], rbuf[0, Q1]) + more[0]
        above = pick(hot[1, 1], rbuf[1, Q1]) + more[1]
        sent(PF, Q1)

        outer_faces(below, above)
        inner_faces()
        for b in (1, 0):
            y = ci[b] + dot(bx[b], vf[b])
            sbuf[1 - b, U2] = y[:F]
            gin[b] = y[:F]
            inn[b] = y[F:]
            send(1 - b, U2)
        inner_faces()
        sbuf[0, Q3] = ci[1, :F] + dot(bx[1, :F, fL], vf[1, fL])
        send(0, Q3)
        sbuf[1, Q3] = ci[0, :F] + dot(bx[0, :F, fU], vf[0, fU])
        send(1, Q3)
        coarse_piece(2 * n + 1)

        more = [ghost(d) for d in (0, 1)]
        arrive(U2)
        outer_faces(rbuf[0, U2], rbuf[1, U2])
        inner_sweep()
        arrive(Q3)
        below = rbuf[0, Q3] + more[0]
        above = rbuf[1, Q3] + more[1]
        sent(U2, Q3)

        outer_faces(below, above)
        inner_faces()
        state[1, U] = cn[1, U] + dot(face[1, U], vf[1])
        state[0, L] = cn[0, L] + dot(face[0, L], vf[0])

        @pl.when(n < STEPS - 1)
        def _():
            send(0, PF)
            send(1, PF)

        state[1, :width - F] = cn[1, :width - F] + dot(face[1, :width - F], vf[1])
        state[0, F:] = cn[0, F:] + dot(face[0, F:], vf[0])

        @pl.when(n < STEPS - 1)
        def _():
            for b in (0, 1):
                y = ci[b] + dot(bx[b], vf[b])
                gin[b] = y[:F]
                inn[b] = y[F:]
        return 0

    def coarse_back():
        return pltpu.make_async_remote_copy(
            src_ref=scoarse, dst_ref=rcoarse, send_sem=csem, recv_sem=rcsem,
            device_id={"cuts": lax.rem(c + nc - 1, nc)}, device_id_type=MESH)

    lax.fori_loop(0, STEPS, step, 0)

    def end(b):
        return pltpu.make_async_remote_copy(
            src_ref=state.at[b], dst_ref=prev.at[0, b], send_sem=esem.at[b], recv_sem=resem.at[b],
            device_id={"cuts": lax.rem(c + 1, nc)}, device_id_type=MESH)

    def jump(o):
        return pltpu.make_async_remote_copy(
            src_ref=hb, dst_ref=hs.at[c], send_sem=hsem.at[o], recv_sem=rhsem.at[c],
            device_id={"cuts": lax.rem(c + o, nc)}, device_id_type=MESH)

    def jump_from(o):
        at = lax.rem(c + nc - o, nc)
        return pltpu.make_async_remote_copy(
            src_ref=hb, dst_ref=hs.at[at], send_sem=hsem.at[o], recv_sem=rhsem.at[at],
            device_id={"cuts": at}, device_id_type=MESH)

    def part(o):
        to = lax.rem(s + o, ns)
        return pltpu.make_async_remote_copy(
            src_ref=zb.at[to], dst_ref=zs.at[s], send_sem=zsem.at[o], recv_sem=rzsem.at[s],
            device_id={"sub": to}, device_id_type=MESH)

    def part_from(o):
        at = lax.rem(s + ns - o, ns)
        return pltpu.make_async_remote_copy(
            src_ref=zb.at[at], dst_ref=zs.at[at], send_sem=zsem.at[o], recv_sem=rzsem.at[at],
            device_id={"sub": at}, device_id_type=MESH)

    @pl.when(c < nc - 1)
    def _():
        coarse_back().wait_recv()

    for b in (0, 1):
        hb[pl.ds(b, 1), :] = jnp.sum(state[b], axis=0, keepdims=True) / width - rcoarse[pl.ds(b, 1), :]
    for o in range(2, nc):
        @pl.when(c + o < nc)
        def _():
            jump(o).start()

    @pl.when(c < nc - 1)
    def _():
        for b in (0, 1):
            end(b).start()

    @pl.when(c > 0)
    def _():
        coarse_back().wait_send()

    for o in range(2, nc):
        @pl.when(c - o >= 0)
        def _():
            jump_from(o).wait_recv()

    z = jnp.dot(rm[...], hs[...].reshape(8 * nc, F), precision=HI, preferred_element_type=f32)
    zb[...] = z.reshape(ns, 8, F)
    for o in range(1, ns):
        part(o).start()
    for o in range(1, ns):
        part_from(o).wait_recv()
    zs[s] = zb[s]
    added = jnp.sum(zs[...], axis=0)

    @pl.when(c == 0)
    def _():
        keep.wait()

    @pl.when(c > 0)
    def _():
        for b in (0, 1):
            end(b).wait_recv()
            prev[0, b] = prev[0, b] + jnp.broadcast_to(added[b:b + 1], (width, F))

    for o in range(2, nc):
        @pl.when(c + o < nc)
        def _():
            jump(o).wait_send()
    for o in range(1, ns):
        part(o).wait_send()

    @pl.when(c < nc - 1)
    def _():
        for b in (0, 1):
            end(b).wait_send()


def solution(mesh):
    ns, nc = mesh.shape["sub"], mesh.shape["cuts"]

    def on_device(start, source, inverse, face_map, trans, partner, cond):
        width, cols = start.shape[2:]
        any_ = pl.BlockSpec(memory_space=pl.ANY)
        vmem = pl.BlockSpec(memory_space=pltpu.VMEM)
        V, S = pltpu.VMEM, pltpu.SemaphoreType.DMA
        scratch = dict(
            partner=pltpu.SMEM(partner.shape, jnp.int32), cond=pltpu.SMEM(cond.shape, f32),
            fmap=V(face_map.shape, jnp.int32), trans=V(trans.shape, f32),
            state=V((2, width, cols), f32), src=V((2, width, cols), bf16), inv=V((2, width, width), bf16),
            face=V((2, width, 2 * F), bf16), rf=V((2, 2 * F, cols), f32), vf=V((2, 2 * F, cols), bf16),
            vi=V((2, width - 2 * F, cols), bf16), cn=V((2, width, cols), f32), ci=V((2, 2 * F, cols), f32),
            bx=V((2, 2 * F, 2 * F), bf16), bi=V((2, 2 * F, width - 2 * F), bf16),
            sbuf=V((2, 4, F, cols), f32), rbuf=V((2, 4, F, cols), f32),
            smt=V((2, 8, F), f32), rmt=V((2, 8, F), f32), sst=V((2, 2, F, cols), f32), rst=V((2, 2, F, cols), f32),
            inn=V((2, F, cols), f32), gin=V((2, F, cols), f32), rg=V((2, F, cols), f32),
            tb=V((2, 2, F, cols), f32), tg=V((2, F, cols), f32),
            hot=V((2, 2, F, F), bf16), ghot=V((2, F, F), bf16), mp=V((2, F, F), bf16),
            scoarse=V((8, cols), f32), rcoarse=V((8, cols), f32),
            hs=V((nc, 8, cols), f32), zb=V((ns, 8, cols), f32), zs=V((ns, 8, cols), f32),
            hb=V((8, cols), f32), gm=V((2 * ns, 2 * ns), f32), rm=V((8 * ns, 8 * nc), f32),
            rw=V((2 * ns, 8 * nc), f32),
            lsem=S((8,)), ssem=S((2, 5)), rsem=S((2, 5)), psem=S((2,)), rpsem=S((2,)),
            fsem=S((2, 8)), rfsem=S((2, 8)), esem=S((2,)), resem=S((2,)),
            csem=S(()), rcsem=S(()), hsem=S((nc,)), rhsem=S((nc,)), zsem=S((ns,)), rzsem=S((ns,)),
        )
        return pl.pallas_call(
            functools.partial(kernel, ns, nc),
            out_shape=pltpu.VMEM(start.shape, f32),
            in_specs=[any_] * 7,
            out_specs=vmem,
            scratch_shapes=list(scratch.values()),
            compiler_params=pltpu.CompilerParams(collective_id=0, has_side_effects=True,
                                                 vmem_limit_bytes=40 * 2**20),
            name="parareal",
        )(*[pltpu.with_memory_space_constraint(a, pltpu.HBM)
            for a in (partner, cond, start, source, inverse, face_map, trans)])

    in_specs = (
        P("cuts", "sub", None, None),
        P("sub", None, None),
        P("sub", None, None),
        P("sub", None, None),
        P("sub", None, None),
        P(),
        P(),
    )
    return jax.shard_map(on_device, mesh=mesh, in_specs=in_specs,
                         out_specs=P("cuts", "sub", None, None), check_vma=False)
```

```python
import functools

import jax
import jax.numpy as jnp
from jax import lax
from jax.experimental import pallas as pl
from jax.experimental.pallas import tpu as pltpu
from jax.sharding import PartitionSpec as P

F = 128
STEPS = 4
PARTS = 4
ROW = 4
MESH = pl.DeviceIdType.MESH
f32, bf16 = jnp.float32, jnp.bfloat16
HI = lax.Precision.HIGHEST
PF, Q1, U2, Q3, MT = range(5)
VIA = (Q1, Q3,)


def dot(a, b):
    return jnp.dot(a, b, preferred_element_type=f32)


def chosen(row):
    places = lax.broadcasted_iota(jnp.int32, (F, F), 0).astype(f32)
    hot = jnp.where(places == jnp.broadcast_to(row, (F, F)), 1.0, 0.0).astype(f32)
    return hot.T.astype(bf16)


def down_rows(row):
    return jnp.broadcast_to(row, (F, F)).T


def pick(hot, x):
    high = x.astype(bf16)
    low = (x - high.astype(f32)).astype(bf16)
    both = dot(hot, jnp.concatenate([high, low], axis=1))
    return both[:, :F] + both[:, F:]


def kernel(ns, nc, partner_h, cond_h, start_h, source_h, inv_h, fmap_h, trans_h, prev,
           partner, cond, fmap, trans,
           state, src, inv, face, rf, vf, vi, cn, ci, bx, bi, sbuf, rbuf, smt, rmt, sst, rst,
           inn, gin, rg, tb, tg, hot, ghot, mp, scoarse, rcoarse, hs, zb, zs, hb, gm, rm, rw,
           held, heldsem, passsem, freesem, lsem, ssem, rsem, psem, rpsem, fsem, rfsem, esem, resem, csem, rcsem, hsem, rhsem, zsem, rzsem):
    c, s = lax.axis_index("cuts"), lax.axis_index("sub")
    width = state.shape[1]
    L, U, I = slice(0, F), slice(width - F, width), slice(F, width - F)
    fL, fU = slice(0, F), slice(F, 2 * F)
    has_below, has_above = s > 0, s < ns - 1

    loads = [
        pltpu.make_async_copy(start_h.at[0], state, lsem.at[0]),
        pltpu.make_async_copy(source_h, src, lsem.at[1]),
        pltpu.make_async_copy(inv_h, inv, lsem.at[2]),
        pltpu.make_async_copy(fmap_h, fmap, lsem.at[4]),
        pltpu.make_async_copy(trans_h, trans, lsem.at[5]),
        pltpu.make_async_copy(partner_h, partner, lsem.at[6]),
        pltpu.make_async_copy(cond_h, cond, lsem.at[7]),
    ]
    for k in (3, 4, 0, 1, 2, 5, 6):
        loads[k].start()

    hs[...] = jnp.zeros_like(hs)
    hb[...] = jnp.zeros_like(hb)
    rcoarse[...] = jnp.zeros_like(rcoarse)

    barrier = pltpu.get_barrier_semaphore()
    for o in range(1, ns):
        pl.semaphore_signal(barrier, inc=1, device_id={"sub": lax.rem(s + o, ns)}, device_id_type=MESH)
    for o in range(1, nc):
        pl.semaphore_signal(barrier, inc=1, device_id={"cuts": lax.rem(c + o, nc)}, device_id_type=MESH)

    def towards(d):
        return lax.rem(s + 1, ns) if d == 0 else lax.rem(s + ns - 1, ns)

    def ext_source(d, i):
        if i == MT:
            return smt.at[d]
        if i == PF:
            return state.at[1, pl.ds(width - F, F)] if d == 0 else state.at[0, pl.ds(0, F)]
        return sbuf.at[d, i]

    def ext(d, i):
        return pltpu.make_async_remote_copy(
            src_ref=ext_source(d, i), dst_ref=rmt.at[d] if i == MT else rbuf.at[d, i], send_sem=ssem.at[d, i], recv_sem=rsem.at[d, i],
            device_id={"sub": towards(d)}, device_id_type=MESH)

    sends = (has_above, has_below)
    recvs = (has_below, has_above)

    odd = lax.rem(c, 2) == 1
    at = lax.rem(s, ROW)
    leaves = (odd & (at == ROW - 1) & has_above, odd & (at == 0) & has_below)
    serves = (odd & (at == 0) & (s + ROW < ns), odd & (at == ROW - 1) & (s >= ROW))

    def part_of(ref, h):
        return ref.at[pl.ds(h * (F // PARTS), F // PARTS)]

    def first_leg(d, i, h):
        step = ns + 1 - ROW if d == 0 else ROW - 1
        return pltpu.make_async_remote_copy(
            src_ref=part_of(ext_source(d, i), h), dst_ref=part_of(held.at[d, i], h),
            send_sem=ssem.at[d, i], recv_sem=heldsem.at[d, i, h],
            device_id={"sub": lax.rem(s + step, ns)}, device_id_type=MESH)

    def second_leg(d, i, h=None):
        step = ROW if d == 0 else ns - ROW
        return pltpu.make_async_remote_copy(
            src_ref=held.at[d, i] if h is None else part_of(held.at[d, i], h),
            dst_ref=rbuf.at[d, i] if h is None else part_of(rbuf.at[d, i], h), send_sem=passsem.at[d, i], recv_sem=rsem.at[d, i],
            device_id={"sub": lax.rem(s + step, ns)}, device_id_type=MESH)

    def pass_on(*which):
        for d in (0, 1):
            @pl.when(serves[d])
            def _():
                for i in which:
                    for h in range(PARTS):
                        first_leg(d, i, h).wait_recv()
                        second_leg(d, i, h).start()

    def granted(n, i):
        for d in (0, 1):
            @pl.when(leaves[d] & (n > 0))
            def _():
                pl.semaphore_wait(freesem.at[d, i], 1)

    def grant(n, i):
        for d in (0, 1):
            source = lax.rem(s + (ROW - 1 if d == 0 else ns + 1 - ROW), ns)

            @pl.when(serves[d] & (n < STEPS - 1))
            def _():
                pl.semaphore_signal(freesem.at[d, i], inc=1, device_id={"sub": source}, device_id_type=MESH)

    def passed_on(*which):
        for d in (0, 1):
            @pl.when(serves[d])
            def _():
                for i in which:
                    second_leg(d, i).wait_send()

    def send(d, *which):
        @pl.when(sends[d] & jnp.logical_not(leaves[d]))
        def _():
            for i in which:
                ext(d, i).start()

        @pl.when(leaves[d])
        def _():
            for i in which:
                if i in VIA:
                    for h in range(PARTS):
                        first_leg(d, i, h).start()
                else:
                    ext(d, i).start()

    def sent(*which):
        for d in (0, 1):
            @pl.when(sends[d])
            def _():
                for i in which:
                    ext(d, i).wait_send()

    def arrive(*which):
        for d in (0, 1):
            @pl.when(recvs[d])
            def _():
                for i in which:
                    ext(d, i).wait_recv()

    group = min(8, nc)
    size = F // group
    own = lax.rem(c, group)

    def piece(ref, d, at):
        return ref.at[d, :, pl.ds(pl.multiple_of(at * size, size), size)]

    def across(d):
        return pltpu.make_async_remote_copy(
            src_ref=piece(sst, d, own), dst_ref=piece(rst, d, own), send_sem=psem.at[d], recv_sem=rpsem.at[d],
            device_id={"sub": towards(d)}, device_id_type=MESH)

    def along(d, o):
        return pltpu.make_async_remote_copy(
            src_ref=piece(rst, d, own), dst_ref=piece(rst, d, own), send_sem=fsem.at[d, o],
            recv_sem=rfsem.at[d, own], device_id={"cuts": c - own + lax.rem(own + o, group)}, device_id_type=MESH)

    def along_from(d, o):
        at = lax.rem(own + group - o, group)
        return pltpu.make_async_remote_copy(
            src_ref=piece(rst, d, at), dst_ref=piece(rst, d, at), send_sem=fsem.at[d, o],
            recv_sem=rfsem.at[d, at], device_id={"cuts": c - own + at}, device_id_type=MESH)

    for d in (0, 1):
        @pl.when(jnp.logical_not(recvs[d]))
        def _():
            rbuf[d] = jnp.zeros(rbuf.shape[1:], f32)
            rmt[d] = jnp.zeros(rmt.shape[1:], f32)
            rst[d] = jnp.zeros(rst.shape[1:], f32)

    loads[3].wait()
    loads[4].wait()
    rows = [[fmap[b, pl.ds(k, 1), :].astype(f32) for k in (0, 1)] for b in (0, 1)]
    trow = [[trans[b, pl.ds(k, 1), :] for k in (0, 1)] for b in (0, 1)]
    smt[...] = jnp.zeros_like(smt)
    smt[0, pl.ds(0, 1), :] = rows[1][1]
    smt[0, pl.ds(1, 1), :] = trow[1][1]
    smt[1, pl.ds(0, 1), :] = rows[0][0]
    smt[1, pl.ds(1, 1), :] = trow[0][0]
    for b in (0, 1):
        for k in (0, 1):
            tb[b, k] = down_rows(trow[b][k])
            hot[b, k] = chosen(rows[b][k])

    loads[0].wait()
    keep = pltpu.make_async_copy(start_h.at[0], prev.at[0], lsem.at[3])

    @pl.when(c == 0)
    def _():
        keep.start()

    loads[1].wait()
    sst[0, 1] = src[1, U].astype(f32)
    sst[1, 1] = src[0, L].astype(f32)
    loads[2].wait()
    sst[0, 0] = inv[1, U, U].astype(f32)
    sst[1, 0] = inv[0, L, L].astype(f32)

    pl.semaphore_wait(barrier, ns - 1 + nc - 1)

    for d in (0, 1):
        @pl.when(sends[d])
        def _():
            across(d).start()

        send(d, MT, PF)

    def own_rows(b):
        rows_of = dot(hot[1, 0], inv[0, U, :]) if b == 0 else dot(hot[0, 1], inv[1, L, :])
        rows_of = rows_of.astype(bf16)
        bx[b, F:, fL] = rows_of[:, L]
        bx[b, F:, fU] = rows_of[:, U]
        bi[b, F:] = rows_of[:, I]

    inn[0] = pick(hot[1, 0], state[0, U])
    inn[1] = pick(hot[0, 1], state[1, L])

    def inner_faces():
        vf[0, fU] = (rf[0, fU] + tb[0, 1] * inn[1]).astype(bf16)
        vf[1, fL] = (rf[1, fL] + tb[1, 0] * inn[0]).astype(bf16)

    def inner_sweep():
        for b in (0, 1):
            inn[b] = ci[b, F:] + dot(bx[b, F:], vf[b])

    def outer_faces(below, above):
        vf[0, fL] = (rf[0, fL] + tb[0, 0] * below).astype(bf16)
        vf[1, fU] = (rf[1, fU] + tb[1, 1] * above).astype(bf16)

    def ghost(d):
        return dot(mp[d], (rg[d] + tg[d] * gin[d]).astype(bf16))

    count = 2 * ns
    ri = lax.broadcasted_iota(jnp.int32, (count, count), 0)
    ki = lax.broadcasted_iota(jnp.int32, (count, count), 1)
    pieces = -(-(nc - 1) // 3)

    def coarse_piece(w):
        @pl.when(w == 1)
        def _():
            def link(b, a):
                q, g = partner[b], cond[b]
                a = a + jnp.where((ri == b) & (ki == q), g, 0.0)
                return a + jnp.where((ri == q) & (ki == b), g, 0.0)

            chain = jnp.where((ri - ki == 1) | (ki - ri == 1), 1.0, 0.0).astype(f32)
            a = lax.fori_loop(0, count, link, chain)
            gm[...] = jnp.where(ri == ki, 1.0 + jnp.sum(a, axis=1, keepdims=True), 0.0) - a

        @pl.when((w >= 1) & (w <= 4))
        def _():
            def pivot(i, a):
                at = (w - 1) * (count // 4) + i
                col = jnp.sum(jnp.where(ki == at, a, 0.0), axis=1, keepdims=True)
                row = jnp.sum(jnp.where(ri == at, a, 0.0), axis=0, keepdims=True)
                d = jnp.sum(jnp.where(ki[:1] == at, row, 0.0), axis=1, keepdims=True)
                inv_d = 1.0 / d
                scaled = row * inv_d
                new = jnp.where(ri == at, scaled, a - col * scaled)
                new = jnp.where(ki == at, col * inv_d, new)
                return jnp.where((ki == at) & (ri == at), -inv_d, new)

            gm[...] = lax.fori_loop(0, count // 4, pivot, gm[...])

        @pl.when(w == 5)
        def _():
            rw[...] = jnp.zeros_like(rw)

        @pl.when(w >= 5)
        def _():
            rr = lax.broadcasted_iota(jnp.int32, rw.shape, 0)
            unit = lax.bitwise_and(lax.broadcasted_iota(jnp.int32, rw.shape, 1), 7)
            slot = lax.shift_right_logical(lax.broadcasted_iota(jnp.int32, rw.shape, 1), 3)

            def power(i, acc):
                k = (8 - w) * pieces - i
                here = (unit < 2) & (rr - unit == 2 * s) & (slot == c - 1 - k)
                return -jnp.dot(gm[...], acc + jnp.where(here, 1.0, 0.0), precision=HI,
                                preferred_element_type=f32)

            rw[...] = lax.fori_loop(0, pieces, power, rw[...])

        @pl.when(w == 7)
        def _():
            pr = lax.broadcasted_iota(jnp.int32, (8 * ns, count), 0)
            pc = lax.broadcasted_iota(jnp.int32, (8 * ns, count), 1)
            half = lax.bitwise_and(pr, 7)
            spread = jnp.where((half < 2) & (2 * lax.shift_right_logical(pr, 3) + half == pc), 1.0, 0.0)
            rm[...] = jnp.dot(spread.astype(f32), rw[...], precision=HI, preferred_element_type=f32)

    def step(n, _):
        for b in (0, 1):
            vi[b] = (state[b, I] + src[b, I].astype(f32)).astype(bf16)
            rf[b, fL] = state[b, L] + src[b, L].astype(f32)
            rf[b, fU] = state[b, U] + src[b, U].astype(f32)
        inner_faces()
        granted(n, Q1)
        cn[1, U] = dot(inv[1, U, I], vi[1])
        sbuf[0, Q1] = cn[1, U] + dot(inv[1, U, L], vf[1, fL])
        send(0, Q1)
        cn[0, L] = dot(inv[0, L, I], vi[0])
        sbuf[1, Q1] = cn[0, L] + dot(inv[0, L, U], vf[0, fU])
        send(1, Q1)

        @pl.when(n == 0)
        def _():
            scoarse[...] = jnp.zeros_like(scoarse)
            for b in (0, 1):
                scoarse[pl.ds(b, 1), :] = jnp.sum(state[b], axis=0, keepdims=True) / width
                own_rows(b)
                face[b, :, fL] = inv[b, :, L]
                face[b, :, fU] = inv[b, :, U]

            @pl.when(c > 0)
            def _():
                coarse_back().start()
            pass_on(Q1)
            arrive(MT)
            for d in (0, 1):
                ghot[d] = chosen(rmt[d, pl.ds(0, 1), :])
                tg[d] = down_rows(rmt[d, pl.ds(1, 1), :])
            for b in (0, 1):
                read = dot(ghot[b], inv[0, L, :] if b == 0 else inv[1, U, :]).astype(bf16)
                bx[b, :F, fL] = read[:, L]
                bx[b, :F, fU] = read[:, U]
                bi[b, :F] = read[:, I]
            gin[0] = pick(ghot[0], state[0, L])
            gin[1] = pick(ghot[1], state[1, U])
            for d in (0, 1):
                @pl.when(recvs[d])
                def _():
                    across(d).wait_recv()
                    for o in range(1, group):
                        along(d, o).start()

        for b in (0, 1):
            ci[b] = dot(bi[b], vi[b])
        cn[0, F:] = dot(inv[0, F:, I], vi[0])
        cn[1, :width - F] = dot(inv[1, :width - F, I], vi[1])
        coarse_piece(2 * n)

        @pl.when(n > 0)
        def _():
            pass_on(Q1)

        arrive(PF)
        outer_faces(pick(hot[0, 0], rbuf[0, PF]), pick(hot[1, 1], rbuf[1, PF]))
        inner_sweep()

        @pl.when(n == 0)
        def _():
            for d in (0, 1):
                @pl.when(sends[d])
                def _():
                    across(d).wait_send()

                @pl.when(recvs[d])
                def _():
                    for o in range(1, group):
                        along_from(d, o).wait_recv()
                    for o in range(1, group):
                        along(d, o).wait_send()
            mp[0] = dot(hot[0, 0], rst[0, 0].astype(bf16)).astype(bf16)
            mp[1] = dot(hot[1, 1], rst[1, 0].astype(bf16)).astype(bf16)
            sent(MT)

            loads[5].wait()
            loads[6].wait()

        for d in (0, 1):
            rg[d] = rbuf[d, PF] + rst[d, 1]
        more = [ghost(d) for d in (0, 1)]
        arrive(Q1)
        below = pick(hot[0, 0], rbuf[0, Q1]) + more[0]
        above = pick(hot[1, 1], rbuf[1, Q1]) + more[1]
        sent(PF, Q1)
        passed_on(Q1)
        grant(n, Q1)

        outer_faces(below, above)
        inner_faces()
        for b in (1, 0):
            y = ci[b] + dot(bx[b], vf[b])
            sbuf[1 - b, U2] = y[:F]
            gin[b] = y[:F]
            inn[b] = y[F:]
            send(1 - b, U2)
        inner_faces()
        granted(n, Q3)
        sbuf[0, Q3] = ci[1, :F] + dot(bx[1, :F, fL], vf[1, fL])
        send(0, Q3)
        sbuf[1, Q3] = ci[0, :F] + dot(bx[0, :F, fU], vf[0, fU])
        send(1, Q3)
        coarse_piece(2 * n + 1)

        more = [ghost(d) for d in (0, 1)]
        pass_on(Q3)
        arrive(U2)
        outer_faces(rbuf[0, U2], rbuf[1, U2])
        inner_sweep()
        arrive(Q3)
        below = rbuf[0, Q3] + more[0]
        above = rbuf[1, Q3] + more[1]
        sent(U2, Q3)
        passed_on(Q3)
        grant(n, Q3)

        outer_faces(below, above)
        inner_faces()
        state[1, U] = cn[1, U] + dot(face[1, U], vf[1])
        state[0, L] = cn[0, L] + dot(face[0, L], vf[0])

        @pl.when(n < STEPS - 1)
        def _():
            send(0, PF)
            send(1, PF)

        state[1, :width - F] = cn[1, :width - F] + dot(face[1, :width - F], vf[1])
        state[0, F:] = cn[0, F:] + dot(face[0, F:], vf[0])

        @pl.when(n < STEPS - 1)
        def _():
            for b in (0, 1):
                y = ci[b] + dot(bx[b], vf[b])
                gin[b] = y[:F]
                inn[b] = y[F:]
        return 0

    def coarse_back():
        return pltpu.make_async_remote_copy(
            src_ref=scoarse, dst_ref=rcoarse, send_sem=csem, recv_sem=rcsem,
            device_id={"cuts": lax.rem(c + nc - 1, nc)}, device_id_type=MESH)

    lax.fori_loop(0, STEPS, step, 0)

    def end(b):
        return pltpu.make_async_remote_copy(
            src_ref=state.at[b], dst_ref=prev.at[0, b], send_sem=esem.at[b], recv_sem=resem.at[b],
            device_id={"cuts": lax.rem(c + 1, nc)}, device_id_type=MESH)

    def jump(o):
        return pltpu.make_async_remote_copy(
            src_ref=hb, dst_ref=hs.at[c], send_sem=hsem.at[o], recv_sem=rhsem.at[c],
            device_id={"cuts": lax.rem(c + o, nc)}, device_id_type=MESH)

    def jump_from(o):
        at = lax.rem(c + nc - o, nc)
        return pltpu.make_async_remote_copy(
            src_ref=hb, dst_ref=hs.at[at], send_sem=hsem.at[o], recv_sem=rhsem.at[at],
            device_id={"cuts": at}, device_id_type=MESH)

    def part(o):
        to = lax.rem(s + o, ns)
        return pltpu.make_async_remote_copy(
            src_ref=zb.at[to], dst_ref=zs.at[s], send_sem=zsem.at[o], recv_sem=rzsem.at[s],
            device_id={"sub": to}, device_id_type=MESH)

    def part_from(o):
        at = lax.rem(s + ns - o, ns)
        return pltpu.make_async_remote_copy(
            src_ref=zb.at[at], dst_ref=zs.at[at], send_sem=zsem.at[o], recv_sem=rzsem.at[at],
            device_id={"sub": at}, device_id_type=MESH)

    @pl.when(c < nc - 1)
    def _():
        coarse_back().wait_recv()

    for b in (0, 1):
        hb[pl.ds(b, 1), :] = jnp.sum(state[b], axis=0, keepdims=True) / width - rcoarse[pl.ds(b, 1), :]
    for o in range(2, nc):
        @pl.when(c + o < nc)
        def _():
            jump(o).start()

    @pl.when(c < nc - 1)
    def _():
        for b in (0, 1):
            end(b).start()

    @pl.when(c > 0)
    def _():
        coarse_back().wait_send()

    for o in range(2, nc):
        @pl.when(c - o >= 0)
        def _():
            jump_from(o).wait_recv()

    z = jnp.dot(rm[...], hs[...].reshape(8 * nc, F), precision=HI, preferred_element_type=f32)
    zb[...] = z.reshape(ns, 8, F)
    for o in range(1, ns):
        part(o).start()
    for o in range(1, ns):
        part_from(o).wait_recv()
    zs[s] = zb[s]
    added = jnp.sum(zs[...], axis=0)

    @pl.when(c == 0)
    def _():
        keep.wait()

    @pl.when(c > 0)
    def _():
        for b in (0, 1):
            end(b).wait_recv()
            prev[0, b] = prev[0, b] + jnp.broadcast_to(added[b:b + 1], (width, F))

    for o in range(2, nc):
        @pl.when(c + o < nc)
        def _():
            jump(o).wait_send()
    for o in range(1, ns):
        part(o).wait_send()

    @pl.when(c < nc - 1)
    def _():
        for b in (0, 1):
            end(b).wait_send()


def solution(mesh):
    ns, nc = mesh.shape["sub"], mesh.shape["cuts"]

    def on_device(start, source, inverse, face_map, trans, partner, cond):
        width, cols = start.shape[2:]
        any_ = pl.BlockSpec(memory_space=pl.ANY)
        vmem = pl.BlockSpec(memory_space=pltpu.VMEM)
        V, S = pltpu.VMEM, pltpu.SemaphoreType.DMA
        scratch = dict(
            partner=pltpu.SMEM(partner.shape, jnp.int32), cond=pltpu.SMEM(cond.shape, f32),
            fmap=V(face_map.shape, jnp.int32), trans=V(trans.shape, f32),
            state=V((2, width, cols), f32), src=V((2, width, cols), bf16), inv=V((2, width, width), bf16),
            face=V((2, width, 2 * F), bf16), rf=V((2, 2 * F, cols), f32), vf=V((2, 2 * F, cols), bf16),
            vi=V((2, width - 2 * F, cols), bf16), cn=V((2, width, cols), f32), ci=V((2, 2 * F, cols), f32),
            bx=V((2, 2 * F, 2 * F), bf16), bi=V((2, 2 * F, width - 2 * F), bf16),
            sbuf=V((2, 4, F, cols), f32), rbuf=V((2, 4, F, cols), f32),
            smt=V((2, 8, F), f32), rmt=V((2, 8, F), f32), sst=V((2, 2, F, cols), f32), rst=V((2, 2, F, cols), f32),
            inn=V((2, F, cols), f32), gin=V((2, F, cols), f32), rg=V((2, F, cols), f32),
            tb=V((2, 2, F, cols), f32), tg=V((2, F, cols), f32),
            hot=V((2, 2, F, F), bf16), ghot=V((2, F, F), bf16), mp=V((2, F, F), bf16),
            scoarse=V((8, cols), f32), rcoarse=V((8, cols), f32),
            hs=V((nc, 8, cols), f32), zb=V((ns, 8, cols), f32), zs=V((ns, 8, cols), f32),
            hb=V((8, cols), f32), gm=V((2 * ns, 2 * ns), f32), rm=V((8 * ns, 8 * nc), f32),
            rw=V((2 * ns, 8 * nc), f32),
            held=V((2, 4, F, cols), f32), heldsem=S((2, 4, PARTS)), passsem=S((2, 4)), freesem=pltpu.SemaphoreType.REGULAR((2, 4)), lsem=S((8,)), ssem=S((2, 5)), rsem=S((2, 5)), psem=S((2,)), rpsem=S((2,)),
            fsem=S((2, 8)), rfsem=S((2, 8)), esem=S((2,)), resem=S((2,)),
            csem=S(()), rcsem=S(()), hsem=S((nc,)), rhsem=S((nc,)), zsem=S((ns,)), rzsem=S((ns,)),
        )
        return pl.pallas_call(
            functools.partial(kernel, ns, nc),
            out_shape=pltpu.VMEM(start.shape, f32),
            in_specs=[any_] * 7,
            out_specs=vmem,
            scratch_shapes=list(scratch.values()),
            compiler_params=pltpu.CompilerParams(collective_id=0, has_side_effects=True,
                                                 vmem_limit_bytes=40 * 2**20),
            name="parareal",
        )(*[pltpu.with_memory_space_constraint(a, pltpu.HBM)
            for a in (partner, cond, start, source, inverse, face_map, trans)])

    in_specs = (
        P("cuts", "sub", None, None),
        P("sub", None, None),
        P("sub", None, None),
        P("sub", None, None),
        P("sub", None, None),
        P(),
        P(),
    )
    return jax.shard_map(on_device, mesh=mesh, in_specs=in_specs,
                         out_specs=P("cuts", "sub", None, None), check_vma=False)
```

```python
import functools

import jax
import jax.numpy as jnp
from jax import lax
from jax.experimental import pallas as pl
from jax.experimental.pallas import tpu as pltpu
from jax.sharding import PartitionSpec as P

F = 128
STEPS = 4
PARTS = 8
ROW = 4
MESH = pl.DeviceIdType.MESH
f32, bf16 = jnp.float32, jnp.bfloat16
HI = lax.Precision.HIGHEST
PF, Q1, U2, Q3, MT = range(5)
VIA = (Q1, Q3,)


def dot(a, b):
    return jnp.dot(a, b, preferred_element_type=f32)


def chosen(row):
    places = lax.broadcasted_iota(jnp.int32, (F, F), 0).astype(f32)
    hot = jnp.where(places == jnp.broadcast_to(row, (F, F)), 1.0, 0.0).astype(f32)
    return hot.T.astype(bf16)


def down_rows(row):
    return jnp.broadcast_to(row, (F, F)).T


def pick(hot, x):
    high = x.astype(bf16)
    low = (x - high.astype(f32)).astype(bf16)
    both = dot(hot, jnp.concatenate([high, low], axis=1))
    return both[:, :F] + both[:, F:]


def kernel(ns, nc, partner_h, cond_h, start_h, source_h, inv_h, fmap_h, trans_h, prev,
           partner, cond, fmap, trans,
           state, src, inv, face, rf, vf, vi, cn, ci, bx, bi, sbuf, rbuf, smt, rmt, sst, rst,
           inn, gin, rg, tb, tg, hot, ghot, mp, scoarse, rcoarse, hs, zb, zs, hb, gm, rm, rw,
           held, heldsem, passsem, freesem, lsem, ssem, rsem, psem, rpsem, fsem, rfsem, esem, resem, csem, rcsem, hsem, rhsem, zsem, rzsem):
    c, s = lax.axis_index("cuts"), lax.axis_index("sub")
    width = state.shape[1]
    L, U, I = slice(0, F), slice(width - F, width), slice(F, width - F)
    fL, fU = slice(0, F), slice(F, 2 * F)
    has_below, has_above = s > 0, s < ns - 1

    loads = [
        pltpu.make_async_copy(start_h.at[0], state, lsem.at[0]),
        pltpu.make_async_copy(source_h, src, lsem.at[1]),
        pltpu.make_async_copy(inv_h, inv, lsem.at[2]),
        pltpu.make_async_copy(fmap_h, fmap, lsem.at[4]),
        pltpu.make_async_copy(trans_h, trans, lsem.at[5]),
        pltpu.make_async_copy(partner_h, partner, lsem.at[6]),
        pltpu.make_async_copy(cond_h, cond, lsem.at[7]),
    ]
    for k in (3, 4, 0, 1, 2, 5, 6):
        loads[k].start()

    hs[...] = jnp.zeros_like(hs)
    hb[...] = jnp.zeros_like(hb)
    rcoarse[...] = jnp.zeros_like(rcoarse)

    barrier = pltpu.get_barrier_semaphore()
    for o in range(1, ns):
        pl.semaphore_signal(barrier, inc=1, device_id={"sub": lax.rem(s + o, ns)}, device_id_type=MESH)
    for o in range(1, nc):
        pl.semaphore_signal(barrier, inc=1, device_id={"cuts": lax.rem(c + o, nc)}, device_id_type=MESH)

    def towards(d):
        return lax.rem(s + 1, ns) if d == 0 else lax.rem(s + ns - 1, ns)

    def ext_source(d, i):
        if i == MT:
            return smt.at[d]
        if i == PF:
            return state.at[1, pl.ds(width - F, F)] if d == 0 else state.at[0, pl.ds(0, F)]
        return sbuf.at[d, i]

    def ext(d, i):
        return pltpu.make_async_remote_copy(
            src_ref=ext_source(d, i), dst_ref=rmt.at[d] if i == MT else rbuf.at[d, i], send_sem=ssem.at[d, i], recv_sem=rsem.at[d, i],
            device_id={"sub": towards(d)}, device_id_type=MESH)

    sends = (has_above, has_below)
    recvs = (has_below, has_above)

    odd = lax.rem(c, 2) == 1
    at = lax.rem(s, ROW)
    leaves = (odd & (at == ROW - 1) & has_above, odd & (at == 0) & has_below)
    serves = (odd & (at == 0) & (s + ROW < ns), odd & (at == ROW - 1) & (s >= ROW))

    def part_of(ref, h):
        return ref.at[pl.ds(h * (F // PARTS), F // PARTS)]

    def first_leg(d, i, h):
        step = ns + 1 - ROW if d == 0 else ROW - 1
        return pltpu.make_async_remote_copy(
            src_ref=part_of(ext_source(d, i), h), dst_ref=part_of(held.at[d, i], h),
            send_sem=ssem.at[d, i], recv_sem=heldsem.at[d, i, h],
            device_id={"sub": lax.rem(s + step, ns)}, device_id_type=MESH)

    def second_leg(d, i, h=None):
        step = ROW if d == 0 else ns - ROW
        return pltpu.make_async_remote_copy(
            src_ref=held.at[d, i] if h is None else part_of(held.at[d, i], h),
            dst_ref=rbuf.at[d, i] if h is None else part_of(rbuf.at[d, i], h), send_sem=passsem.at[d, i], recv_sem=rsem.at[d, i],
            device_id={"sub": lax.rem(s + step, ns)}, device_id_type=MESH)

    def pass_on(*which):
        for d in (0, 1):
            @pl.when(serves[d])
            def _():
                for i in which:
                    for h in range(PARTS):
                        first_leg(d, i, h).wait_recv()
                        second_leg(d, i, h).start()

    def granted(n, i):
        for d in (0, 1):
            @pl.when(leaves[d] & (n > 0))
            def _():
                pl.semaphore_wait(freesem.at[d, i], 1)

    def grant(n, i):
        for d in (0, 1):
            source = lax.rem(s + (ROW - 1 if d == 0 else ns + 1 - ROW), ns)

            @pl.when(serves[d] & (n < STEPS - 1))
            def _():
                pl.semaphore_signal(freesem.at[d, i], inc=1, device_id={"sub": source}, device_id_type=MESH)

    def passed_on(*which):
        for d in (0, 1):
            @pl.when(serves[d])
            def _():
                for i in which:
                    second_leg(d, i).wait_send()

    def send(d, *which):
        @pl.when(sends[d] & jnp.logical_not(leaves[d]))
        def _():
            for i in which:
                ext(d, i).start()

        @pl.when(leaves[d])
        def _():
            for i in which:
                if i in VIA:
                    for h in range(PARTS):
                        first_leg(d, i, h).start()
                else:
                    ext(d, i).start()

    def sent(*which):
        for d in (0, 1):
            @pl.when(sends[d])
            def _():
                for i in which:
                    ext(d, i).wait_send()

    def arrive(*which):
        for d in (0, 1):
            @pl.when(recvs[d])
            def _():
                for i in which:
                    ext(d, i).wait_recv()

    group = min(8, nc)
    size = F // group
    own = lax.rem(c, group)

    def piece(ref, d, at):
        return ref.at[d, :, pl.ds(pl.multiple_of(at * size, size), size)]

    def across(d):
        return pltpu.make_async_remote_copy(
            src_ref=piece(sst, d, own), dst_ref=piece(rst, d, own), send_sem=psem.at[d], recv_sem=rpsem.at[d],
            device_id={"sub": towards(d)}, device_id_type=MESH)

    def along(d, o):
        return pltpu.make_async_remote_copy(
            src_ref=piece(rst, d, own), dst_ref=piece(rst, d, own), send_sem=fsem.at[d, o],
            recv_sem=rfsem.at[d, own], device_id={"cuts": c - own + lax.rem(own + o, group)}, device_id_type=MESH)

    def along_from(d, o):
        at = lax.rem(own + group - o, group)
        return pltpu.make_async_remote_copy(
            src_ref=piece(rst, d, at), dst_ref=piece(rst, d, at), send_sem=fsem.at[d, o],
            recv_sem=rfsem.at[d, at], device_id={"cuts": c - own + at}, device_id_type=MESH)

    for d in (0, 1):
        @pl.when(jnp.logical_not(recvs[d]))
        def _():
            rbuf[d] = jnp.zeros(rbuf.shape[1:], f32)
            rmt[d] = jnp.zeros(rmt.shape[1:], f32)
            rst[d] = jnp.zeros(rst.shape[1:], f32)

    loads[3].wait()
    loads[4].wait()
    rows = [[fmap[b, pl.ds(k, 1), :].astype(f32) for k in (0, 1)] for b in (0, 1)]
    trow = [[trans[b, pl.ds(k, 1), :] for k in (0, 1)] for b in (0, 1)]
    smt[...] = jnp.zeros_like(smt)
    smt[0, pl.ds(0, 1), :] = rows[1][1]
    smt[0, pl.ds(1, 1), :] = trow[1][1]
    smt[1, pl.ds(0, 1), :] = rows[0][0]
    smt[1, pl.ds(1, 1), :] = trow[0][0]
    for b in (0, 1):
        for k in (0, 1):
            tb[b, k] = down_rows(trow[b][k])
            hot[b, k] = chosen(rows[b][k])

    loads[0].wait()
    keep = pltpu.make_async_copy(start_h.at[0], prev.at[0], lsem.at[3])

    @pl.when(c == 0)
    def _():
        keep.start()

    loads[1].wait()
    sst[0, 1] = src[1, U].astype(f32)
    sst[1, 1] = src[0, L].astype(f32)
    loads[2].wait()
    sst[0, 0] = inv[1, U, U].astype(f32)
    sst[1, 0] = inv[0, L, L].astype(f32)

    pl.semaphore_wait(barrier, ns - 1 + nc - 1)

    for d in (0, 1):
        @pl.when(sends[d])
        def _():
            across(d).start()

        send(d, MT, PF)

    def own_rows(b):
        rows_of = dot(hot[1, 0], inv[0, U, :]) if b == 0 else dot(hot[0, 1], inv[1, L, :])
        rows_of = rows_of.astype(bf16)
        bx[b, F:, fL] = rows_of[:, L]
        bx[b, F:, fU] = rows_of[:, U]
        bi[b, F:] = rows_of[:, I]

    inn[0] = pick(hot[1, 0], state[0, U])
    inn[1] = pick(hot[0, 1], state[1, L])

    def inner_faces():
        vf[0, fU] = (rf[0, fU] + tb[0, 1] * inn[1]).astype(bf16)
        vf[1, fL] = (rf[1, fL] + tb[1, 0] * inn[0]).astype(bf16)

    def inner_sweep():
        for b in (0, 1):
            inn[b] = ci[b, F:] + dot(bx[b, F:], vf[b])

    def outer_faces(below, above):
        vf[0, fL] = (rf[0, fL] + tb[0, 0] * below).astype(bf16)
        vf[1, fU] = (rf[1, fU] + tb[1, 1] * above).astype(bf16)

    def ghost(d):
        return dot(mp[d], (rg[d] + tg[d] * gin[d]).astype(bf16))

    count = 2 * ns
    ri = lax.broadcasted_iota(jnp.int32, (count, count), 0)
    ki = lax.broadcasted_iota(jnp.int32, (count, count), 1)
    pieces = -(-(nc - 1) // 3)

    def coarse_piece(w):
        @pl.when(w == 1)
        def _():
            def link(b, a):
                q, g = partner[b], cond[b]
                a = a + jnp.where((ri == b) & (ki == q), g, 0.0)
                return a + jnp.where((ri == q) & (ki == b), g, 0.0)

            chain = jnp.where((ri - ki == 1) | (ki - ri == 1), 1.0, 0.0).astype(f32)
            a = lax.fori_loop(0, count, link, chain)
            gm[...] = jnp.where(ri == ki, 1.0 + jnp.sum(a, axis=1, keepdims=True), 0.0) - a

        @pl.when((w >= 1) & (w <= 4))
        def _():
            def pivot(i, a):
                at = (w - 1) * (count // 4) + i
                col = jnp.sum(jnp.where(ki == at, a, 0.0), axis=1, keepdims=True)
                row = jnp.sum(jnp.where(ri == at, a, 0.0), axis=0, keepdims=True)
                d = jnp.sum(jnp.where(ki[:1] == at, row, 0.0), axis=1, keepdims=True)
                inv_d = 1.0 / d
                scaled = row * inv_d
                new = jnp.where(ri == at, scaled, a - col * scaled)
                new = jnp.where(ki == at, col * inv_d, new)
                return jnp.where((ki == at) & (ri == at), -inv_d, new)

            gm[...] = lax.fori_loop(0, count // 4, pivot, gm[...])

        @pl.when(w == 5)
        def _():
            rw[...] = jnp.zeros_like(rw)

        @pl.when(w >= 5)
        def _():
            rr = lax.broadcasted_iota(jnp.int32, rw.shape, 0)
            unit = lax.bitwise_and(lax.broadcasted_iota(jnp.int32, rw.shape, 1), 7)
            slot = lax.shift_right_logical(lax.broadcasted_iota(jnp.int32, rw.shape, 1), 3)

            def power(i, acc):
                k = (8 - w) * pieces - i
                here = (unit < 2) & (rr - unit == 2 * s) & (slot == c - 1 - k)
                return -jnp.dot(gm[...], acc + jnp.where(here, 1.0, 0.0), precision=HI,
                                preferred_element_type=f32)

            rw[...] = lax.fori_loop(0, pieces, power, rw[...])

        @pl.when(w == 7)
        def _():
            pr = lax.broadcasted_iota(jnp.int32, (8 * ns, count), 0)
            pc = lax.broadcasted_iota(jnp.int32, (8 * ns, count), 1)
            half = lax.bitwise_and(pr, 7)
            spread = jnp.where((half < 2) & (2 * lax.shift_right_logical(pr, 3) + half == pc), 1.0, 0.0)
            rm[...] = jnp.dot(spread.astype(f32), rw[...], precision=HI, preferred_element_type=f32)

    def step(n, _):
        for b in (0, 1):
            vi[b] = (state[b, I] + src[b, I].astype(f32)).astype(bf16)
            rf[b, fL] = state[b, L] + src[b, L].astype(f32)
            rf[b, fU] = state[b, U] + src[b, U].astype(f32)
        inner_faces()
        granted(n, Q1)
        cn[1, U] = dot(inv[1, U, I], vi[1])
        sbuf[0, Q1] = cn[1, U] + dot(inv[1, U, L], vf[1, fL])
        send(0, Q1)
        cn[0, L] = dot(inv[0, L, I], vi[0])
        sbuf[1, Q1] = cn[0, L] + dot(inv[0, L, U], vf[0, fU])
        send(1, Q1)

        @pl.when(n == 0)
        def _():
            scoarse[...] = jnp.zeros_like(scoarse)
            for b in (0, 1):
                scoarse[pl.ds(b, 1), :] = jnp.sum(state[b], axis=0, keepdims=True) / width
                own_rows(b)
                face[b, :, fL] = inv[b, :, L]
                face[b, :, fU] = inv[b, :, U]

            @pl.when(c > 0)
            def _():
                coarse_back().start()
            for d in (0, 1):
                @pl.when(recvs[d])
                def _():
                    across(d).wait_recv()
                    for o in range(1, group):
                        along(d, o).start()
            pass_on(Q1)
            arrive(MT)
            for d in (0, 1):
                ghot[d] = chosen(rmt[d, pl.ds(0, 1), :])
                tg[d] = down_rows(rmt[d, pl.ds(1, 1), :])
            for b in (0, 1):
                read = dot(ghot[b], inv[0, L, :] if b == 0 else inv[1, U, :]).astype(bf16)
                bx[b, :F, fL] = read[:, L]
                bx[b, :F, fU] = read[:, U]
                bi[b, :F] = read[:, I]
            gin[0] = pick(ghot[0], state[0, L])
            gin[1] = pick(ghot[1], state[1, U])

        for b in (0, 1):
            ci[b] = dot(bi[b], vi[b])
        cn[0, F:] = dot(inv[0, F:, I], vi[0])
        cn[1, :width - F] = dot(inv[1, :width - F, I], vi[1])
        coarse_piece(2 * n)

        @pl.when(n > 0)
        def _():
            pass_on(Q1)

        arrive(PF)
        outer_faces(pick(hot[0, 0], rbuf[0, PF]), pick(hot[1, 1], rbuf[1, PF]))
        inner_sweep()

        @pl.when(n == 0)
        def _():
            for d in (0, 1):
                @pl.when(sends[d])
                def _():
                    across(d).wait_send()

                @pl.when(recvs[d])
                def _():
                    for o in range(1, group):
                        along_from(d, o).wait_recv()
                    for o in range(1, group):
                        along(d, o).wait_send()
            mp[0] = dot(hot[0, 0], rst[0, 0].astype(bf16)).astype(bf16)
            mp[1] = dot(hot[1, 1], rst[1, 0].astype(bf16)).astype(bf16)
            sent(MT)

            loads[5].wait()
            loads[6].wait()

        for d in (0, 1):
            rg[d] = rbuf[d, PF] + rst[d, 1]
        more = [ghost(d) for d in (0, 1)]
        arrive(Q1)
        below = pick(hot[0, 0], rbuf[0, Q1]) + more[0]
        above = pick(hot[1, 1], rbuf[1, Q1]) + more[1]
        sent(PF, Q1)
        passed_on(Q1)
        grant(n, Q1)

        outer_faces(below, above)
        inner_faces()
        for b in (1, 0):
            y = ci[b] + dot(bx[b], vf[b])
            sbuf[1 - b, U2] = y[:F]
            gin[b] = y[:F]
            inn[b] = y[F:]
        inner_faces()
        granted(n, Q3)
        sbuf[0, Q3] = ci[1, :F] + dot(bx[1, :F, fL], vf[1, fL])
        sbuf[1, Q3] = ci[0, :F] + dot(bx[0, :F, fU], vf[0, fU])
        for d in (0, 1):
            send(d, U2, Q3)
        coarse_piece(2 * n + 1)

        more = [ghost(d) for d in (0, 1)]
        pass_on(Q3)
        arrive(U2)
        outer_faces(rbuf[0, U2], rbuf[1, U2])
        inner_sweep()
        arrive(Q3)
        below = rbuf[0, Q3] + more[0]
        above = rbuf[1, Q3] + more[1]
        sent(U2, Q3)
        passed_on(Q3)
        grant(n, Q3)

        outer_faces(below, above)
        inner_faces()
        state[1, U] = cn[1, U] + dot(face[1, U], vf[1])
        state[0, L] = cn[0, L] + dot(face[0, L], vf[0])

        @pl.when(n < STEPS - 1)
        def _():
            send(0, PF)
            send(1, PF)

        state[1, :width - F] = cn[1, :width - F] + dot(face[1, :width - F], vf[1])
        state[0, F:] = cn[0, F:] + dot(face[0, F:], vf[0])

        @pl.when(n < STEPS - 1)
        def _():
            for b in (0, 1):
                y = ci[b] + dot(bx[b], vf[b])
                gin[b] = y[:F]
                inn[b] = y[F:]
        return 0

    def coarse_back():
        return pltpu.make_async_remote_copy(
            src_ref=scoarse, dst_ref=rcoarse, send_sem=csem, recv_sem=rcsem,
            device_id={"cuts": lax.rem(c + nc - 1, nc)}, device_id_type=MESH)

    lax.fori_loop(0, STEPS, step, 0)

    def end(b):
        return pltpu.make_async_remote_copy(
            src_ref=state.at[b], dst_ref=prev.at[0, b], send_sem=esem.at[b], recv_sem=resem.at[b],
            device_id={"cuts": lax.rem(c + 1, nc)}, device_id_type=MESH)

    def jump(o):
        return pltpu.make_async_remote_copy(
            src_ref=hb, dst_ref=hs.at[c], send_sem=hsem.at[o], recv_sem=rhsem.at[c],
            device_id={"cuts": lax.rem(c + o, nc)}, device_id_type=MESH)

    def jump_from(o):
        at = lax.rem(c + nc - o, nc)
        return pltpu.make_async_remote_copy(
            src_ref=hb, dst_ref=hs.at[at], send_sem=hsem.at[o], recv_sem=rhsem.at[at],
            device_id={"cuts": at}, device_id_type=MESH)

    def part(o):
        to = lax.rem(s + o, ns)
        return pltpu.make_async_remote_copy(
            src_ref=zb.at[to], dst_ref=zs.at[s], send_sem=zsem.at[o], recv_sem=rzsem.at[s],
            device_id={"sub": to}, device_id_type=MESH)

    def part_from(o):
        at = lax.rem(s + ns - o, ns)
        return pltpu.make_async_remote_copy(
            src_ref=zb.at[at], dst_ref=zs.at[at], send_sem=zsem.at[o], recv_sem=rzsem.at[at],
            device_id={"sub": at}, device_id_type=MESH)

    @pl.when(c < nc - 1)
    def _():
        coarse_back().wait_recv()

    for b in (0, 1):
        hb[pl.ds(b, 1), :] = jnp.sum(state[b], axis=0, keepdims=True) / width - rcoarse[pl.ds(b, 1), :]
    for o in range(2, nc):
        @pl.when(c + o < nc)
        def _():
            jump(o).start()

    @pl.when(c < nc - 1)
    def _():
        for b in (0, 1):
            end(b).start()

    @pl.when(c > 0)
    def _():
        coarse_back().wait_send()

    for o in range(2, nc):
        @pl.when(c - o >= 0)
        def _():
            jump_from(o).wait_recv()

    z = jnp.dot(rm[...], hs[...].reshape(8 * nc, F), precision=HI, preferred_element_type=f32)
    zb[...] = z.reshape(ns, 8, F)
    for o in range(1, ns):
        part(o).start()
    for o in range(1, ns):
        part_from(o).wait_recv()
    zs[s] = zb[s]
    added = jnp.sum(zs[...], axis=0)

    @pl.when(c == 0)
    def _():
        keep.wait()

    @pl.when(c > 0)
    def _():
        for b in (0, 1):
            end(b).wait_recv()
            prev[0, b] = prev[0, b] + jnp.broadcast_to(added[b:b + 1], (width, F))

    for o in range(2, nc):
        @pl.when(c + o < nc)
        def _():
            jump(o).wait_send()
    for o in range(1, ns):
        part(o).wait_send()

    @pl.when(c < nc - 1)
    def _():
        for b in (0, 1):
            end(b).wait_send()


def solution(mesh):
    ns, nc = mesh.shape["sub"], mesh.shape["cuts"]

    def on_device(start, source, inverse, face_map, trans, partner, cond):
        width, cols = start.shape[2:]
        any_ = pl.BlockSpec(memory_space=pl.ANY)
        vmem = pl.BlockSpec(memory_space=pltpu.VMEM)
        V, S = pltpu.VMEM, pltpu.SemaphoreType.DMA
        scratch = dict(
            partner=pltpu.SMEM(partner.shape, jnp.int32), cond=pltpu.SMEM(cond.shape, f32),
            fmap=V(face_map.shape, jnp.int32), trans=V(trans.shape, f32),
            state=V((2, width, cols), f32), src=V((2, width, cols), bf16), inv=V((2, width, width), bf16),
            face=V((2, width, 2 * F), bf16), rf=V((2, 2 * F, cols), f32), vf=V((2, 2 * F, cols), bf16),
            vi=V((2, width - 2 * F, cols), bf16), cn=V((2, width, cols), f32), ci=V((2, 2 * F, cols), f32),
            bx=V((2, 2 * F, 2 * F), bf16), bi=V((2, 2 * F, width - 2 * F), bf16),
            sbuf=V((2, 4, F, cols), f32), rbuf=V((2, 4, F, cols), f32),
            smt=V((2, 8, F), f32), rmt=V((2, 8, F), f32), sst=V((2, 2, F, cols), f32), rst=V((2, 2, F, cols), f32),
            inn=V((2, F, cols), f32), gin=V((2, F, cols), f32), rg=V((2, F, cols), f32),
            tb=V((2, 2, F, cols), f32), tg=V((2, F, cols), f32),
            hot=V((2, 2, F, F), bf16), ghot=V((2, F, F), bf16), mp=V((2, F, F), bf16),
            scoarse=V((8, cols), f32), rcoarse=V((8, cols), f32),
            hs=V((nc, 8, cols), f32), zb=V((ns, 8, cols), f32), zs=V((ns, 8, cols), f32),
            hb=V((8, cols), f32), gm=V((2 * ns, 2 * ns), f32), rm=V((8 * ns, 8 * nc), f32),
            rw=V((2 * ns, 8 * nc), f32),
            held=V((2, 4, F, cols), f32), heldsem=S((2, 4, PARTS)), passsem=S((2, 4)), freesem=pltpu.SemaphoreType.REGULAR((2, 4)), lsem=S((8,)), ssem=S((2, 5)), rsem=S((2, 5)), psem=S((2,)), rpsem=S((2,)),
            fsem=S((2, 8)), rfsem=S((2, 8)), esem=S((2,)), resem=S((2,)),
            csem=S(()), rcsem=S(()), hsem=S((nc,)), rhsem=S((nc,)), zsem=S((ns,)), rzsem=S((ns,)),
        )
        return pl.pallas_call(
            functools.partial(kernel, ns, nc),
            out_shape=pltpu.VMEM(start.shape, f32),
            in_specs=[any_] * 7,
            out_specs=vmem,
            scratch_shapes=list(scratch.values()),
            compiler_params=pltpu.CompilerParams(collective_id=0, has_side_effects=True,
                                                 vmem_limit_bytes=40 * 2**20),
            name="parareal",
        )(*[pltpu.with_memory_space_constraint(a, pltpu.HBM)
            for a in (partner, cond, start, source, inverse, face_map, trans)])

    in_specs = (
        P("cuts", "sub", None, None),
        P("sub", None, None),
        P("sub", None, None),
        P("sub", None, None),
        P("sub", None, None),
        P(),
        P(),
    )
    return jax.shard_map(on_device, mesh=mesh, in_specs=in_specs,
                         out_specs=P("cuts", "sub", None, None), check_vma=False)
```

```python
import functools

import jax
import jax.numpy as jnp
from jax import lax
from jax.experimental import pallas as pl
from jax.experimental.pallas import tpu as pltpu
from jax.sharding import PartitionSpec as P

F = 128
STEPS = 4
PARTS = 8
ROW = 4
MESH = pl.DeviceIdType.MESH
f32, bf16 = jnp.float32, jnp.bfloat16
HI = lax.Precision.HIGHEST
PF, Q1, U2, Q3, MT = range(5)
VIA = (Q1, Q3,)


def dot(a, b):
    return jnp.dot(a, b, preferred_element_type=f32)


def chosen(row):
    places = lax.broadcasted_iota(jnp.int32, (F, F), 0).astype(f32)
    hot = jnp.where(places == jnp.broadcast_to(row, (F, F)), 1.0, 0.0).astype(f32)
    return hot.T.astype(bf16)


def down_rows(row):
    return jnp.broadcast_to(row, (F, F)).T


def pick(hot, x):
    high = x.astype(bf16)
    low = (x - high.astype(f32)).astype(bf16)
    both = dot(hot, jnp.concatenate([high, low], axis=1))
    return both[:, :F] + both[:, F:]


def kernel(ns, nc, partner_h, cond_h, start_h, source_h, inv_h, fmap_h, trans_h, prev,
           partner, cond, fmap, trans,
           state, src, inv, face, rf, vf, vi, cn, ci, bx, bi, sbuf, rbuf, smt, rmt, sst, rst,
           inn, gin, rg, tb, tg, hot, ghot, mp, scoarse, rcoarse, hs, zb, zs, hb, gm, rm, rw,
           held, heldsem, passsem, freesem, lsem, ssem, rsem, psem, rpsem, fsem, rfsem, esem, resem, csem, rcsem, hsem, rhsem, zsem, rzsem):
    c, s = lax.axis_index("cuts"), lax.axis_index("sub")
    width = state.shape[1]
    L, U, I = slice(0, F), slice(width - F, width), slice(F, width - F)
    fL, fU = slice(0, F), slice(F, 2 * F)
    has_below, has_above = s > 0, s < ns - 1

    loads = [
        pltpu.make_async_copy(start_h.at[0], state, lsem.at[0]),
        pltpu.make_async_copy(source_h, src, lsem.at[1]),
        pltpu.make_async_copy(inv_h, inv, lsem.at[2]),
        pltpu.make_async_copy(fmap_h, fmap, lsem.at[4]),
        pltpu.make_async_copy(trans_h, trans, lsem.at[5]),
        pltpu.make_async_copy(partner_h, partner, lsem.at[6]),
        pltpu.make_async_copy(cond_h, cond, lsem.at[7]),
    ]
    for k in (3, 4, 0, 1, 2, 5, 6):
        loads[k].start()

    hs[...] = jnp.zeros_like(hs)
    hb[...] = jnp.zeros_like(hb)
    rcoarse[...] = jnp.zeros_like(rcoarse)

    barrier = pltpu.get_barrier_semaphore()
    for o in range(1, ns):
        pl.semaphore_signal(barrier, inc=1, device_id={"sub": lax.rem(s + o, ns)}, device_id_type=MESH)
    for o in range(1, nc):
        pl.semaphore_signal(barrier, inc=1, device_id={"cuts": lax.rem(c + o, nc)}, device_id_type=MESH)

    def towards(d):
        return lax.rem(s + 1, ns) if d == 0 else lax.rem(s + ns - 1, ns)

    def ext_source(d, i):
        if i == MT:
            return smt.at[d]
        if i == PF:
            return state.at[1, pl.ds(width - F, F)] if d == 0 else state.at[0, pl.ds(0, F)]
        return sbuf.at[d, i]

    def ext(d, i):
        return pltpu.make_async_remote_copy(
            src_ref=ext_source(d, i), dst_ref=rmt.at[d] if i == MT else rbuf.at[d, i], send_sem=ssem.at[d, i], recv_sem=rsem.at[d, i],
            device_id={"sub": towards(d)}, device_id_type=MESH)

    sends = (has_above, has_below)
    recvs = (has_below, has_above)

    odd = lax.rem(c, 2) == 1
    at = lax.rem(s, ROW)
    leaves = (odd & (at == ROW - 1) & has_above, odd & (at == 0) & has_below)
    serves = (odd & (at == 0) & (s + ROW < ns), odd & (at == ROW - 1) & (s >= ROW))

    def part_of(ref, h):
        return ref.at[pl.ds(h * (F // PARTS), F // PARTS)]

    def first_leg(d, i, h):
        step = ns + 1 - ROW if d == 0 else ROW - 1
        return pltpu.make_async_remote_copy(
            src_ref=part_of(ext_source(d, i), h), dst_ref=part_of(held.at[d, i], h),
            send_sem=ssem.at[d, i], recv_sem=heldsem.at[d, i, h],
            device_id={"sub": lax.rem(s + step, ns)}, device_id_type=MESH)

    def second_leg(d, i, h=None):
        step = ROW if d == 0 else ns - ROW
        return pltpu.make_async_remote_copy(
            src_ref=held.at[d, i] if h is None else part_of(held.at[d, i], h),
            dst_ref=rbuf.at[d, i] if h is None else part_of(rbuf.at[d, i], h), send_sem=passsem.at[d, i], recv_sem=rsem.at[d, i],
            device_id={"sub": lax.rem(s + step, ns)}, device_id_type=MESH)

    def pass_on(*which):
        for d in (0, 1):
            @pl.when(serves[d])
            def _():
                for i in which:
                    for h in range(PARTS):
                        first_leg(d, i, h).wait_recv()
                        second_leg(d, i, h).start()

    def granted(n, i):
        for d in (0, 1):
            @pl.when(leaves[d] & (n > 0))
            def _():
                pl.semaphore_wait(freesem.at[d, i], 1)

    def grant(n, i):
        for d in (0, 1):
            source = lax.rem(s + (ROW - 1 if d == 0 else ns + 1 - ROW), ns)

            @pl.when(serves[d] & (n < STEPS - 1))
            def _():
                pl.semaphore_signal(freesem.at[d, i], inc=1, device_id={"sub": source}, device_id_type=MESH)

    def passed_on(*which):
        for d in (0, 1):
            @pl.when(serves[d])
            def _():
                for i in which:
                    second_leg(d, i).wait_send()

    def send(d, *which):
        @pl.when(sends[d] & jnp.logical_not(leaves[d]))
        def _():
            for i in which:
                ext(d, i).start()

        @pl.when(leaves[d])
        def _():
            for i in which:
                if i in VIA:
                    for h in range(PARTS):
                        first_leg(d, i, h).start()
                else:
                    ext(d, i).start()

    def sent(*which):
        for d in (0, 1):
            @pl.when(sends[d])
            def _():
                for i in which:
                    ext(d, i).wait_send()

    def arrive(*which):
        for d in (0, 1):
            @pl.when(recvs[d])
            def _():
                for i in which:
                    ext(d, i).wait_recv()

    group = min(8, nc)
    size = F // group
    own = lax.rem(c, group)

    def piece(ref, d, at):
        return ref.at[d, :, pl.ds(pl.multiple_of(at * size, size), size)]

    def across(d):
        return pltpu.make_async_remote_copy(
            src_ref=piece(sst, d, own), dst_ref=piece(rst, d, own), send_sem=psem.at[d], recv_sem=rpsem.at[d],
            device_id={"sub": towards(d)}, device_id_type=MESH)

    def along(d, o):
        return pltpu.make_async_remote_copy(
            src_ref=piece(rst, d, own), dst_ref=piece(rst, d, own), send_sem=fsem.at[d, o],
            recv_sem=rfsem.at[d, own], device_id={"cuts": c - own + lax.rem(own + o, group)}, device_id_type=MESH)

    def along_from(d, o):
        at = lax.rem(own + group - o, group)
        return pltpu.make_async_remote_copy(
            src_ref=piece(rst, d, at), dst_ref=piece(rst, d, at), send_sem=fsem.at[d, o],
            recv_sem=rfsem.at[d, at], device_id={"cuts": c - own + at}, device_id_type=MESH)

    for d in (0, 1):
        @pl.when(jnp.logical_not(recvs[d]))
        def _():
            rbuf[d] = jnp.zeros(rbuf.shape[1:], f32)
            rmt[d] = jnp.zeros(rmt.shape[1:], f32)
            rst[d] = jnp.zeros(rst.shape[1:], f32)

    loads[3].wait()
    loads[4].wait()
    rows = [[fmap[b, pl.ds(k, 1), :].astype(f32) for k in (0, 1)] for b in (0, 1)]
    trow = [[trans[b, pl.ds(k, 1), :] for k in (0, 1)] for b in (0, 1)]
    smt[...] = jnp.zeros_like(smt)
    smt[0, pl.ds(0, 1), :] = rows[1][1]
    smt[0, pl.ds(1, 1), :] = trow[1][1]
    smt[1, pl.ds(0, 1), :] = rows[0][0]
    smt[1, pl.ds(1, 1), :] = trow[0][0]
    for b in (0, 1):
        for k in (0, 1):
            tb[b, k] = down_rows(trow[b][k])
            hot[b, k] = chosen(rows[b][k])

    loads[0].wait()
    keep = pltpu.make_async_copy(start_h.at[0], prev.at[0], lsem.at[3])

    @pl.when(c == 0)
    def _():
        keep.start()

    loads[1].wait()
    sst[0, 1] = src[1, U].astype(f32)
    sst[1, 1] = src[0, L].astype(f32)
    loads[2].wait()
    sst[0, 0] = inv[1, U, U].astype(f32)
    sst[1, 0] = inv[0, L, L].astype(f32)

    pl.semaphore_wait(barrier, ns - 1 + nc - 1)

    for d in (0, 1):
        @pl.when(sends[d])
        def _():
            across(d).start()

        send(d, MT, PF)

    def own_rows(b):
        rows_of = dot(hot[1, 0], inv[0, U, :]) if b == 0 else dot(hot[0, 1], inv[1, L, :])
        rows_of = rows_of.astype(bf16)
        bx[b, F:, fL] = rows_of[:, L]
        bx[b, F:, fU] = rows_of[:, U]
        bi[b, F:] = rows_of[:, I]

    inn[0] = pick(hot[1, 0], state[0, U])
    inn[1] = pick(hot[0, 1], state[1, L])

    def inner_faces():
        vf[0, fU] = (rf[0, fU] + tb[0, 1] * inn[1]).astype(bf16)
        vf[1, fL] = (rf[1, fL] + tb[1, 0] * inn[0]).astype(bf16)

    def inner_sweep():
        for b in (0, 1):
            inn[b] = ci[b, F:] + dot(bx[b, F:], vf[b])

    def outer_faces(below, above):
        vf[0, fL] = (rf[0, fL] + tb[0, 0] * below).astype(bf16)
        vf[1, fU] = (rf[1, fU] + tb[1, 1] * above).astype(bf16)

    def ghost(d):
        return dot(mp[d], (rg[d] + tg[d] * gin[d]).astype(bf16))

    count = 2 * ns
    ri = lax.broadcasted_iota(jnp.int32, (count, count), 0)
    ki = lax.broadcasted_iota(jnp.int32, (count, count), 1)
    pieces = -(-(nc - 1) // 3)

    def coarse_piece(w):
        @pl.when(w == 1)
        def _():
            def link(b, a):
                q, g = partner[b], cond[b]
                a = a + jnp.where((ri == b) & (ki == q), g, 0.0)
                return a + jnp.where((ri == q) & (ki == b), g, 0.0)

            chain = jnp.where((ri - ki == 1) | (ki - ri == 1), 1.0, 0.0).astype(f32)
            a = lax.fori_loop(0, count, link, chain)
            gm[...] = jnp.where(ri == ki, 1.0 + jnp.sum(a, axis=1, keepdims=True), 0.0) - a

        @pl.when((w >= 1) & (w <= 4))
        def _():
            def pivot(i, a):
                at = (w - 1) * (count // 4) + i
                col = jnp.sum(jnp.where(ki == at, a, 0.0), axis=1, keepdims=True)
                row = jnp.sum(jnp.where(ri == at, a, 0.0), axis=0, keepdims=True)
                d = jnp.sum(jnp.where(ki[:1] == at, row, 0.0), axis=1, keepdims=True)
                inv_d = 1.0 / d
                scaled = row * inv_d
                new = jnp.where(ri == at, scaled, a - col * scaled)
                new = jnp.where(ki == at, col * inv_d, new)
                return jnp.where((ki == at) & (ri == at), -inv_d, new)

            gm[...] = lax.fori_loop(0, count // 4, pivot, gm[...])

        @pl.when(w == 5)
        def _():
            rw[...] = jnp.zeros_like(rw)

        @pl.when(w >= 5)
        def _():
            rr = lax.broadcasted_iota(jnp.int32, rw.shape, 0)
            unit = lax.bitwise_and(lax.broadcasted_iota(jnp.int32, rw.shape, 1), 7)
            slot = lax.shift_right_logical(lax.broadcasted_iota(jnp.int32, rw.shape, 1), 3)

            def power(i, acc):
                k = (8 - w) * pieces - i
                here = (unit < 2) & (rr - unit == 2 * s) & (slot == c - 1 - k)
                return -jnp.dot(gm[...], acc + jnp.where(here, 1.0, 0.0), precision=HI,
                                preferred_element_type=f32)

            rw[...] = lax.fori_loop(0, pieces, power, rw[...])

        @pl.when(w == 7)
        def _():
            pr = lax.broadcasted_iota(jnp.int32, (8 * ns, count), 0)
            pc = lax.broadcasted_iota(jnp.int32, (8 * ns, count), 1)
            half = lax.bitwise_and(pr, 7)
            spread = jnp.where((half < 2) & (2 * lax.shift_right_logical(pr, 3) + half == pc), 1.0, 0.0)
            rm[...] = jnp.dot(spread.astype(f32), rw[...], precision=HI, preferred_element_type=f32)

    def step(n, _):
        for b in (0, 1):
            vi[b] = (state[b, I] + src[b, I].astype(f32)).astype(bf16)
            rf[b, fL] = state[b, L] + src[b, L].astype(f32)
            rf[b, fU] = state[b, U] + src[b, U].astype(f32)
        inner_faces()
        granted(n, Q1)
        cn[1, U] = dot(inv[1, U, I], vi[1])
        sbuf[0, Q1] = cn[1, U] + dot(inv[1, U, L], vf[1, fL])
        send(0, Q1)
        cn[0, L] = dot(inv[0, L, I], vi[0])
        sbuf[1, Q1] = cn[0, L] + dot(inv[0, L, U], vf[0, fU])
        send(1, Q1)

        @pl.when(n == 0)
        def _():
            scoarse[...] = jnp.zeros_like(scoarse)
            for b in (0, 1):
                scoarse[pl.ds(b, 1), :] = jnp.sum(state[b], axis=0, keepdims=True) / width
                own_rows(b)
                face[b, :, fL] = inv[b, :, L]
                face[b, :, fU] = inv[b, :, U]

            @pl.when(c > 0)
            def _():
                coarse_back().start()
            for d in (0, 1):
                @pl.when(recvs[d])
                def _():
                    across(d).wait_recv()
                    for o in range(1, group):
                        along(d, o).start()
            pass_on(Q1)
            arrive(MT)
            for d in (0, 1):
                ghot[d] = chosen(rmt[d, pl.ds(0, 1), :])
                tg[d] = down_rows(rmt[d, pl.ds(1, 1), :])
            for b in (0, 1):
                read = dot(ghot[b], inv[0, L, :] if b == 0 else inv[1, U, :]).astype(bf16)
                bx[b, :F, fL] = read[:, L]
                bx[b, :F, fU] = read[:, U]
                bi[b, :F] = read[:, I]
            gin[0] = pick(ghot[0], state[0, L])
            gin[1] = pick(ghot[1], state[1, U])

        for b in (0, 1):
            ci[b] = dot(bi[b], vi[b])
        cn[0, F:] = dot(inv[0, F:, I], vi[0])
        cn[1, :width - F] = dot(inv[1, :width - F, I], vi[1])
        coarse_piece(2 * n)

        @pl.when(n > 0)
        def _():
            pass_on(Q1)

        arrive(PF)
        outer_faces(pick(hot[0, 0], rbuf[0, PF]), pick(hot[1, 1], rbuf[1, PF]))
        inner_sweep()

        @pl.when(n == 0)
        def _():
            for d in (0, 1):
                @pl.when(sends[d])
                def _():
                    across(d).wait_send()

                @pl.when(recvs[d])
                def _():
                    for o in range(1, group):
                        along_from(d, o).wait_recv()
                    for o in range(1, group):
                        along(d, o).wait_send()
            mp[0] = dot(hot[0, 0], rst[0, 0].astype(bf16)).astype(bf16)
            mp[1] = dot(hot[1, 1], rst[1, 0].astype(bf16)).astype(bf16)
            sent(MT)

            loads[5].wait()
            loads[6].wait()

        for d in (0, 1):
            rg[d] = rbuf[d, PF] + rst[d, 1]
        more = [ghost(d) for d in (0, 1)]
        arrive(Q1)
        below = pick(hot[0, 0], rbuf[0, Q1]) + more[0]
        above = pick(hot[1, 1], rbuf[1, Q1]) + more[1]
        sent(PF, Q1)
        passed_on(Q1)
        grant(n, Q1)

        outer_faces(below, above)
        inner_faces()
        for b in (1, 0):
            y = ci[b] + dot(bx[b], vf[b])
            sbuf[1 - b, U2] = y[:F]
            gin[b] = y[:F]
            inn[b] = y[F:]
        inner_faces()
        granted(n, Q3)
        sbuf[0, Q3] = ci[1, :F] + dot(bx[1, :F, fL], vf[1, fL])
        sbuf[1, Q3] = ci[0, :F] + dot(bx[0, :F, fU], vf[0, fU])
        for d in (0, 1):
            send(d, U2, Q3)
        coarse_piece(2 * n + 1)

        more = [ghost(d) for d in (0, 1)]
        pass_on(Q3)
        arrive(U2)
        outer_faces(rbuf[0, U2], rbuf[1, U2])
        inner_sweep()
        arrive(Q3)
        below = rbuf[0, Q3] + more[0]
        above = rbuf[1, Q3] + more[1]
        sent(U2, Q3)
        passed_on(Q3)
        grant(n, Q3)

        outer_faces(below, above)
        inner_faces()
        state[1, U] = cn[1, U] + dot(face[1, U], vf[1])
        state[0, L] = cn[0, L] + dot(face[0, L], vf[0])

        @pl.when(n < STEPS - 1)
        def _():
            send(0, PF)
            send(1, PF)

        state[1, :width - F] = cn[1, :width - F] + dot(face[1, :width - F], vf[1])
        state[0, F:] = cn[0, F:] + dot(face[0, F:], vf[0])

        @pl.when(n < STEPS - 1)
        def _():
            for b in (0, 1):
                y = ci[b] + dot(bx[b], vf[b])
                gin[b] = y[:F]
                inn[b] = y[F:]
        return 0

    def coarse_back():
        return pltpu.make_async_remote_copy(
            src_ref=scoarse, dst_ref=rcoarse, send_sem=csem, recv_sem=rcsem,
            device_id={"cuts": lax.rem(c + nc - 1, nc)}, device_id_type=MESH)

    lax.fori_loop(0, STEPS, step, 0)

    def end(b):
        return pltpu.make_async_remote_copy(
            src_ref=state.at[b], dst_ref=prev.at[0, b], send_sem=esem.at[b], recv_sem=resem.at[b],
            device_id={"cuts": lax.rem(c + 1, nc)}, device_id_type=MESH)

    def jump(o):
        return pltpu.make_async_remote_copy(
            src_ref=hb, dst_ref=hs.at[c], send_sem=hsem.at[o], recv_sem=rhsem.at[c],
            device_id={"cuts": lax.rem(c + o, nc)}, device_id_type=MESH)

    def jump_from(o):
        at = lax.rem(c + nc - o, nc)
        return pltpu.make_async_remote_copy(
            src_ref=hb, dst_ref=hs.at[at], send_sem=hsem.at[o], recv_sem=rhsem.at[at],
            device_id={"cuts": at}, device_id_type=MESH)

    def part(o):
        to = lax.rem(s + o, ns)
        return pltpu.make_async_remote_copy(
            src_ref=zb.at[to], dst_ref=zs.at[s], send_sem=zsem.at[o], recv_sem=rzsem.at[s],
            device_id={"sub": to}, device_id_type=MESH)

    def part_from(o):
        at = lax.rem(s + ns - o, ns)
        return pltpu.make_async_remote_copy(
            src_ref=zb.at[at], dst_ref=zs.at[at], send_sem=zsem.at[o], recv_sem=rzsem.at[at],
            device_id={"sub": at}, device_id_type=MESH)

    @pl.when(c < nc - 1)
    def _():
        coarse_back().wait_recv()

    for b in (0, 1):
        hb[pl.ds(b, 1), :] = jnp.sum(state[b], axis=0, keepdims=True) / width - rcoarse[pl.ds(b, 1), :]
    for o in reversed(range(2, nc)):
        @pl.when(c + o < nc)
        def _():
            jump(o).start()

    @pl.when(c < nc - 1)
    def _():
        for b in (0, 1):
            end(b).start()

    @pl.when(c > 0)
    def _():
        coarse_back().wait_send()

    for o in range(2, nc):
        @pl.when(c - o >= 0)
        def _():
            jump_from(o).wait_recv()

    z = jnp.dot(rm[...], hs[...].reshape(8 * nc, F), precision=HI, preferred_element_type=f32)
    zb[...] = z.reshape(ns, 8, F)
    for o in sorted(range(1, ns), key=lambda o: -min(o, ns - o)):
        part(o).start()
    for o in range(1, ns):
        part_from(o).wait_recv()
    zs[s] = zb[s]
    added = jnp.sum(zs[...], axis=0)

    @pl.when(c == 0)
    def _():
        keep.wait()

    @pl.when(c > 0)
    def _():
        for b in (0, 1):
            end(b).wait_recv()
            prev[0, b] = prev[0, b] + jnp.broadcast_to(added[b:b + 1], (width, F))

    for o in range(2, nc):
        @pl.when(c + o < nc)
        def _():
            jump(o).wait_send()
    for o in range(1, ns):
        part(o).wait_send()

    @pl.when(c < nc - 1)
    def _():
        for b in (0, 1):
            end(b).wait_send()


def solution(mesh):
    ns, nc = mesh.shape["sub"], mesh.shape["cuts"]

    def on_device(start, source, inverse, face_map, trans, partner, cond):
        width, cols = start.shape[2:]
        any_ = pl.BlockSpec(memory_space=pl.ANY)
        vmem = pl.BlockSpec(memory_space=pltpu.VMEM)
        V, S = pltpu.VMEM, pltpu.SemaphoreType.DMA
        scratch = dict(
            partner=pltpu.SMEM(partner.shape, jnp.int32), cond=pltpu.SMEM(cond.shape, f32),
            fmap=V(face_map.shape, jnp.int32), trans=V(trans.shape, f32),
            state=V((2, width, cols), f32), src=V((2, width, cols), bf16), inv=V((2, width, width), bf16),
            face=V((2, width, 2 * F), bf16), rf=V((2, 2 * F, cols), f32), vf=V((2, 2 * F, cols), bf16),
            vi=V((2, width - 2 * F, cols), bf16), cn=V((2, width, cols), f32), ci=V((2, 2 * F, cols), f32),
            bx=V((2, 2 * F, 2 * F), bf16), bi=V((2, 2 * F, width - 2 * F), bf16),
            sbuf=V((2, 4, F, cols), f32), rbuf=V((2, 4, F, cols), f32),
            smt=V((2, 8, F), f32), rmt=V((2, 8, F), f32), sst=V((2, 2, F, cols), f32), rst=V((2, 2, F, cols), f32),
            inn=V((2, F, cols), f32), gin=V((2, F, cols), f32), rg=V((2, F, cols), f32),
            tb=V((2, 2, F, cols), f32), tg=V((2, F, cols), f32),
            hot=V((2, 2, F, F), bf16), ghot=V((2, F, F), bf16), mp=V((2, F, F), bf16),
            scoarse=V((8, cols), f32), rcoarse=V((8, cols), f32),
            hs=V((nc, 8, cols), f32), zb=V((ns, 8, cols), f32), zs=V((ns, 8, cols), f32),
            hb=V((8, cols), f32), gm=V((2 * ns, 2 * ns), f32), rm=V((8 * ns, 8 * nc), f32),
            rw=V((2 * ns, 8 * nc), f32),
            held=V((2, 4, F, cols), f32), heldsem=S((2, 4, PARTS)), passsem=S((2, 4)), freesem=pltpu.SemaphoreType.REGULAR((2, 4)), lsem=S((8,)), ssem=S((2, 5)), rsem=S((2, 5)), psem=S((2,)), rpsem=S((2,)),
            fsem=S((2, 8)), rfsem=S((2, 8)), esem=S((2,)), resem=S((2,)),
            csem=S(()), rcsem=S(()), hsem=S((nc,)), rhsem=S((nc,)), zsem=S((ns,)), rzsem=S((ns,)),
        )
        return pl.pallas_call(
            functools.partial(kernel, ns, nc),
            out_shape=pltpu.VMEM(start.shape, f32),
            in_specs=[any_] * 7,
            out_specs=vmem,
            scratch_shapes=list(scratch.values()),
            compiler_params=pltpu.CompilerParams(collective_id=0, has_side_effects=True,
                                                 vmem_limit_bytes=40 * 2**20),
            name="parareal",
        )(*[pltpu.with_memory_space_constraint(a, pltpu.HBM)
            for a in (partner, cond, start, source, inverse, face_map, trans)])

    in_specs = (
        P("cuts", "sub", None, None),
        P("sub", None, None),
        P("sub", None, None),
        P("sub", None, None),
        P("sub", None, None),
        P(),
        P(),
    )
    return jax.shard_map(on_device, mesh=mesh, in_specs=in_specs,
                         out_specs=P("cuts", "sub", None, None), check_vma=False)
```
